32 devices in a mesh: depth: 16 (over z, y, x), spec: 2 (over core).
Axes of the slice: x: 2, y: 2, z: 4, core: 2. Of those that a mesh axis runs over, the one named last changes fastest.
Arguments:
- emission: bfloat16 [512, 64, 2048], P('depth', 'spec'), may hold values from 0.099609375 to 2
- opacity: bfloat16 [512, 64, 2048], P('depth', 'spec'), may hold values from 0.29882812 to 3
- bin_extinction: float32 [64], P('spec'), may hold values from 0.1 to 30
- entry: int32 [2048], replicated, may hold values from 0 to 127
- exit_cell: int32 [2048], replicated, may hold values from 384 to 512
- response: float32 [3, 64], P(None, 'spec'), may hold values from 0.05 to 1
Outputs:
- nearer_slab_rgb: float32 [16, 3, 2048], P('depth')
- image: float32 [3, 2048], replicated
The draws below stay inside these ranges and needn't reach their ends.
All inputs are finite; a program needn't handle non-finite values.
Results may differ from the reference program's by a relative error of at most 0.0003.
Values sent between devices are 32-bit elements; how exact they have to be, the bound alone decides.
A program may use at most 64 MiB of HBM per device.

```python
import math
import jax
import jax.numpy as jnp
from jax import lax

BINS = 64
CZ = 32
RAYS = 2048
DEPTH_SLABS = 16
NZ = 512


def place_ends(result, key, low, top_value):
    longest = result.shape.index(max(result.shape))
    spots = []
    for shift in (0, 1):
        where = [jax.random.randint(jax.random.fold_in(key, axis), (), 0, length) for axis, length in enumerate(result.shape)]
        where[longest] = (where[longest] + shift) % result.shape[longest]
        spots.append(tuple(where))
    return result.at[spots[0]].set(low).at[spots[1]].set(top_value)


def block_levels(rng, shape, cuts, least, largest):
    def one(axis_at, blocks):
        steps = jax.random.uniform(jax.random.fold_in(jax.random.fold_in(rng, 6), axis_at), (blocks,), jnp.float32, least / len(cuts), largest / len(cuts))
        return jnp.repeat(jnp.exp(steps), shape[axis_at] // blocks).reshape((-1,) + (1,) * (len(shape) - axis_at - 1))

    loudness = one(*cuts[0])
    for cut in cuts[1:]:
        loudness = loudness * one(*cut)
    return loudness


def setup_inputs(seed: int = 0) -> dict:
    key_list = jax.random.split(jax.random.key(seed), 7)
    emission = jnp.clip(jnp.exp(math.log(2.0) - 2.9996462 * jax.random.uniform(key_list[0], (NZ, BINS, RAYS), jnp.float32) ** block_levels(key_list[0], (NZ, BINS, RAYS), ((0, 16), (1, 2)), -0.2, 0.2)), 0.099609375, 2.0).astype(jnp.bfloat16)
    opacity = jnp.clip(jnp.exp(math.log(3.0) - 2.306499 * jax.random.uniform(key_list[1], (NZ, BINS, RAYS), jnp.float32) ** block_levels(key_list[1], (NZ, BINS, RAYS), ((0, 16), (1, 2)), -0.2, 0.2)), 0.29882812, 3.0).astype(jnp.bfloat16)
    bin_extinction = jnp.clip(jnp.exp(math.log(30.0) - 5.7037825 * jax.random.uniform(key_list[2], (BINS,), jnp.float32) ** block_levels(key_list[2], (BINS,), ((0, 2),), -0.2, 0.2)), 0.1, 30.0)
    entry = place_ends(jax.random.randint(key_list[3], (RAYS,), 0, NZ // 4), jax.random.fold_in(key_list[3], 1), 0, (NZ // 4) - 1).astype(jnp.int32)
    exit_cell = place_ends(jax.random.randint(key_list[4], (RAYS,), 3 * NZ // 4, NZ + 1), jax.random.fold_in(key_list[4], 1), 3 * NZ // 4, NZ).astype(jnp.int32)
    response = jnp.clip(0.05 + 0.95 * jax.random.uniform(key_list[5], (3, BINS), jnp.float32) ** block_levels(key_list[5], (3, BINS), ((1, 2),), -0.2, 0.2), 0.05, 1.0)
    return dict(emission=emission, opacity=opacity, bin_extinction=bin_extinction, entry=entry, exit_cell=exit_cell, response=response)


def merge_slabs(earlier, later):
    return (earlier[0] + earlier[1] * later[0], earlier[1] * later[1])


def reference(emission, opacity, bin_extinction, entry, exit_cell, response):
    cell_step = 1.0 / NZ
    emitted = emission.reshape(DEPTH_SLABS, CZ, BINS, RAYS)
    absorbed = opacity.reshape(DEPTH_SLABS, CZ, BINS, RAYS)

    def section_pass(inputs):
        glow, dense, section = inputs
        depth = section * CZ + jnp.arange(CZ, dtype=jnp.int32)
        inside = (depth[:, None] >= entry[None, :]) & (depth[:, None] < exit_cell[None, :])
        live = jnp.where(inside, 1.0, 0.0).astype(jnp.float32)
        tau = bin_extinction[None, :, None] * dense.astype(jnp.float32) * live[:, None, :] * cell_step
        running = jnp.cumsum(tau, axis=0)
        before = running - tau
        light = jnp.sum(glow.astype(jnp.float32) * live[:, None, :] * cell_step * jnp.exp(-before), axis=0)
        trans = jnp.exp(-(before[-1] + tau[-1]))
        return light, trans

    slab_radiances, transes = lax.map(section_pass, (emitted, absorbed, jnp.arange(DEPTH_SLABS, dtype=jnp.int32)))

    def advance(carry, pair):
        return merge_slabs(carry, pair), carry

    start = (jnp.zeros((BINS, RAYS), jnp.float32), jnp.ones((BINS, RAYS), jnp.float32))
    unused, fronts = lax.scan(advance, start, (slab_radiances, transes))
    nearer_radiance, nearer_transparency = fronts
    nearer_slab_rgb = jnp.einsum("ol,vlm->vom", response, nearer_radiance, precision=lax.Precision.HIGHEST)
    slab_colour_rgb = jnp.einsum("ol,vlm->vom", response, nearer_transparency * slab_radiances, precision=lax.Precision.HIGHEST)
    image = jnp.sum(slab_colour_rgb, axis=0)
    return nearer_slab_rgb, image
```

```python
import functools
import math
import jax
import jax.numpy as jnp
from jax import lax
from jax.experimental import pallas as pl
from jax.experimental.pallas import tpu as pltpu
from jax.sharding import PartitionSpec as P

LANES = 128
SUBLANES = 8
MESH = pl.DeviceIdType.MESH


def padded(colours):
    return -(-colours // 4) * 4


def column(row, eye):
    return jnp.sum(jnp.where(eye, row, 0.0), axis=1, keepdims=True)


def kernel(
    groups, members, specs,
    em_hbm, op_hbm, ext_hbm, entry_hbm, exit_hbm, resp_hbm,
    near_ref, image_ref,
    em_v, op_v, ext_v, entry_v, exit_v, resp_v, w_own, w_all,
    s_out, s_in, l_out, l_in, d_out, d_in, f_out, f_in, x_out, x_in,
    em_sem, op_sem, small_sem, w_send, w_recv,
    s_send, s_recv, l_send, l_recv, d_send, d_recv, f_send, f_recv, x_send, x_recv, ready,
):
    cells, bins, rays = em_hbm.shape
    colours = resp_hbm.shape[0]
    tiles = rays // (members * LANES)
    half = rays // tiles
    rows = padded(colours)
    sections = groups * members
    cell_step = 1.0 / (cells * sections)
    me = lax.axis_index("depth")
    spec = lax.axis_index("spec")
    g = me // members
    mi = me % members
    lead = specs - 1
    is_lead = spec == lead
    last = members - 1
    paired = members & (members - 1) == 0

    def owner(t):
        if not paired:
            return (mi + 1 + t) % members
        if isinstance(t, int):
            mask = 0 if t == last else (t + 1) // 2 if t % 2 else last - t // 2
        else:
            odd = t % 2
            mask = jnp.where(t == last, 0, odd * ((t + 1) // 2) + (1 - odd) * (last - t // 2))
        who = 0
        bit = 1
        while bit < members:
            who = who + ((mi // bit + mask // bit) % 2) * bit
            bit *= 2
        return who

    def core(group, member, s):
        return (group * members + member, s)

    def read(hbm, vmem, sem, j):
        at = pl.ds(j * half, half)
        return pltpu.make_async_copy(hbm.at[:, :, at], vmem.at[:, :, at], sem.at[j])

    for j in range(tiles):
        read(op_hbm, op_v, op_sem, j).start()
    small = [
        pltpu.make_async_copy(hbm, vmem, small_sem.at[n])
        for n, (hbm, vmem) in enumerate(
            ((entry_hbm, entry_v), (exit_hbm, exit_v), (ext_hbm, ext_v), (resp_hbm, resp_v))
        )
    ]
    for copy in small:
        copy.start()

    barrier = pltpu.get_barrier_semaphore()
    near_barrier = groups == 2
    if near_barrier:
        other = 1 - g

        @pl.when(is_lead)
        def _():
            for t in range(members):
                for s in range(specs):
                    if t < last or s != lead:
                        pl.semaphore_signal(
                            barrier, inc=1, device_id=core(g, owner(t), s), device_id_type=MESH
                        )
            pl.semaphore_signal(barrier, inc=1, device_id=core(other, mi, lead), device_id_type=MESH)
    else:
        @pl.loop(1, sections * specs)
        def _(n):
            index = (me * specs + spec + n) % (sections * specs)
            pl.semaphore_signal(
                barrier, inc=1, device_id=(index // specs, index % specs), device_id_type=MESH
            )

    for j in range(tiles):
        read(em_hbm, em_v, em_sem, j).start()

    def enter():
        if near_barrier:
            @pl.when(is_lead)
            def _():
                pl.semaphore_wait(barrier, members)

            @pl.when(spec != lead)
            def _():
                pl.semaphore_wait(barrier, members)
        else:
            pl.semaphore_wait(barrier, sections * specs - 1)

    for copy in small:
        copy.wait()

    eye = lax.broadcasted_iota(jnp.int32, (bins, bins), 0) == lax.broadcasted_iota(
        jnp.int32, (bins, bins), 1
    )
    scale = column(ext_v[...].reshape(1, bins), eye) * (-cell_step * math.log2(math.e))
    scale = jnp.broadcast_to(scale, (bins, LANES))
    for c in range(colours):
        w_own[c] = jnp.broadcast_to(column(resp_v[pl.ds(c, 1), :], eye), (bins, LANES))
    x_out[...] = jnp.zeros_like(x_out)
    f_out[...] = jnp.zeros_like(f_out)
    first = me * cells

    def lanes(j, q):
        return pl.ds(pl.multiple_of((j * members + q) * LANES, LANES), LANES)

    def bounds(at):
        low = jnp.broadcast_to(entry_v[at].reshape(1, LANES) - first, (SUBLANES, LANES))
        high = jnp.broadcast_to(exit_v[at].reshape(1, LANES) - first, (SUBLANES, LANES))
        return low, high

    def live_at(i, low, high):
        return jnp.where((low <= i) & (high > i), 1.0, 0.0)

    def masked(x, live):
        x = x.astype(jnp.float32).reshape(bins // SUBLANES, SUBLANES, LANES)
        return (x * live[None]).reshape(bins, LANES)

    def depth_of(j, t):
        at = lanes(j, owner(t))
        low, high = bounds(at)
        total = jnp.zeros((bins, LANES), jnp.float32)
        for i in range(cells):
            total = total + masked(op_v[i, :, at], live_at(i, low, high))
        s_out[j, t] = total * scale

    def light_of(j, t):
        at = lanes(j, owner(t))
        low, high = bounds(at)
        run = jnp.zeros((bins, LANES), jnp.float32)
        glow = jnp.zeros((bins, LANES), jnp.float32)
        for i in range(cells):
            live = live_at(i, low, high)
            glow = glow + masked(em_v[i, :, at], live) * jnp.exp2(run)
            run = run + masked(op_v[i, :, at], live) * scale
        l_out[j, t] = glow * cell_step

    def piece(out, into, send, recv, j, t):
        return pltpu.make_async_remote_copy(
            out.at[j, t], into.at[j, mi, spec], send.at[j, t], recv.at[j, mi, spec],
            device_id=core(g, owner(t), lead), device_id_type=MESH,
        )

    def leaves(t):
        return (t < last) | (spec != lead)

    depth_args = (s_out, s_in, s_send, s_recv)
    light_args = (l_out, l_in, l_send, l_recv)

    def send(args, j, t):
        @pl.when(leaves(t))
        def _():
            piece(*args, j, t).start()

        @pl.when((t == last) & is_lead)
        def _():
            args[1][j, mi, spec] = args[0][j, t]

    w_copies = [
        pltpu.make_async_remote_copy(
            w_own, w_all.at[spec], w_send, w_recv.at[spec],
            device_id=(me, lead), device_id_type=MESH,
        )
    ]

    for j in range(tiles):
        read(op_hbm, op_v, op_sem, j).wait()
        if j == 0:
            @pl.loop(0, members)
            def _(t):
                depth_of(0, t)

            enter()

            @pl.loop(0, members)
            def _(t):
                send(depth_args, 0, t)
        else:
            @pl.loop(0, members)
            def _(t):
                depth_of(j, t)
                send(depth_args, j, t)

    @pl.when(is_lead)
    def _():
        w_all[lead] = w_own[...]

    @pl.when(spec != lead)
    def _():
        w_copies[0].start()

    for j in range(tiles):
        read(em_hbm, em_v, em_sem, j).wait()

        @pl.loop(0, members)
        def _(t):
            light_of(j, t)
            send(light_args, j, t)

    def arrive(args, j):
        out, into, send_sem, recv_sem = args
        for t in range(members):
            for s in range(specs):
                if t < last or s != lead:
                    k = owner(t)
                    pltpu.make_async_remote_copy(
                        out.at[j, t], into.at[j, k, s], send_sem.at[j, t], recv_sem.at[j, k, s],
                        device_id=core(g, k, s), device_id_type=MESH,
                    ).wait_recv()

    def chain(j):
        return pltpu.make_async_remote_copy(
            d_out.at[j], d_in.at[j], d_send.at[j], d_recv.at[j],
            device_id=core((g + 1) % groups, mi, lead), device_id_type=MESH,
        )

    def total_copy(dg, t, s):
        return pltpu.make_async_remote_copy(
            x_out, x_in.at[g, mi], x_send.at[dg - 1, t, s], x_recv.at[g, mi],
            device_id=core((g + dg) % groups, owner(t), s), device_id_type=MESH,
        )

    def block_copy(t, s):
        k = owner(t)
        return pltpu.make_async_remote_copy(
            f_out.at[k], f_in.at[mi], f_send.at[t, s], f_recv.at[mi],
            device_id=core(g, k, s), device_id_type=MESH,
        )

    @pl.when(is_lead)
    def _():
        for j in range(tiles):
            arrive(depth_args, j)

            @pl.when(g == 0)
            def _():
                d_in[j] = jnp.zeros(d_in.shape[1:], jnp.float32)

            if groups > 1:
                @pl.when(g < groups - 1)
                def _():
                    here = s_in[j, 0]
                    for k in range(1, members):
                        here = here + s_in[j, k]
                    if groups > 2:
                        @pl.when(g > 0)
                        def _():
                            chain(j).wait_recv()

                        here = here + d_in[j]
                    d_out[j] = here
                    chain(j).start()

        if near_barrier:
            @pl.when(g == 1)
            def _():
                pl.semaphore_signal(ready, inc=1, device_id=core(0, mi, lead), device_id_type=MESH)

        for s in range(specs):
            if s != lead:
                pltpu.make_async_remote_copy(
                    w_own, w_all.at[s], w_send, w_recv.at[s], device_id=(me, s), device_id_type=MESH,
                ).wait_recv()

        for j in range(tiles):
            arrive(light_args, j)
            if groups > 1:
                @pl.when((g > 0) if groups == 2 else (g == groups - 1))
                def _():
                    chain(j).wait_recv()

            ahead = d_in[j]
            sums = [jnp.zeros((SUBLANES, LANES), jnp.float32) for _ in range(colours)]
            for k in range(members):
                seen = jnp.exp2(ahead) * l_in[j, k]
                for c in range(colours):
                    if k > 0:
                        f_out[k, 0, pl.ds(rows * j + c, 1), :] = jnp.sum(sums[c], axis=0, keepdims=True)
                    part = (seen * w_all[:, c]).reshape(-1, SUBLANES, LANES)
                    sums[c] = sums[c] + jnp.sum(part, axis=0)
                if k < members - 1:
                    ahead = ahead + s_in[j, k]
            for c in range(colours):
                x_out[pl.ds(rows * j + c, 1), :] = jnp.sum(sums[c], axis=0, keepdims=True)

        if near_barrier:
            @pl.when(g == 0)
            def _():
                pl.semaphore_wait(ready, 1)

        for dg in range(1, groups):
            for t in range(members):
                for s in range(specs):
                    total_copy(dg, t, s).start()
        for k in range(members):
            f_out[k, 1] = x_out[...]
        for t in range(members):
            for s in range(specs):
                if t < last or s != lead:
                    block_copy(t, s).start()
        f_in[mi] = f_out[mi]

    for t in range(members):
        q = owner(t)

        @pl.when(leaves(t))
        def _():
            pltpu.make_async_remote_copy(
                f_out.at[0], f_in.at[q], f_send.at[t, 0], f_recv.at[q],
                device_id=core(g, q, lead), device_id_type=MESH,
            ).wait_recv()

    for dg in range(1, groups):
        src = (g + dg) % groups
        for q in range(members):
            pltpu.make_async_remote_copy(
                x_out, x_in.at[src, q], x_send.at[0, 0, 0], x_recv.at[src, q],
                device_id=core(src, q, lead), device_id_type=MESH,
            ).wait_recv()

    for q in range(members):
        near = f_in[q, 0]
        image = f_in[q, 1]
        for dg in range(1, groups):
            src = (g + dg) % groups
            value = x_in[src, q]
            near = near + value * jnp.where(src < g, 1.0, 0.0)
            image = image + value
        for j in range(tiles):
            at = pl.ds((j * members + q) * LANES, LANES)
            near_ref[0, :, at] = near[4 * j:rows * j + colours]
            image_ref[:, at] = image[4 * j:rows * j + colours]

    for args in (depth_args, light_args):
        for j in range(tiles):
            @pl.loop(0, members)
            def _(t):
                @pl.when(leaves(t))
                def _():
                    piece(*args, j, t).wait_send()

    @pl.when(spec != lead)
    def _():
        w_copies[0].wait_send()

    @pl.when(is_lead)
    def _():
        for j in range(tiles):
            if groups > 1:
                @pl.when(g < groups - 1)
                def _():
                    chain(j).wait_send()
        for t in range(members):
            for s in range(specs):
                for dg in range(1, groups):
                    total_copy(dg, t, s).wait_send()
                if t < last or s != lead:
                    block_copy(t, s).wait_send()


def place(near_ref, image_ref, near_out, image_out):
    for c in range(near_out.shape[0]):
        near_out[c] = near_ref[:, c]
    image_out[...] = image_ref[...]


def body(groups, members, specs, emission, opacity, bin_extinction, entry, exit_cell, response):
    cells, bins, rays = emission.shape
    colours = response.shape[0]
    tiles = rays // (members * LANES)
    rows = padded(colours)
    f32 = jnp.float32
    vmem = pl.BlockSpec(memory_space=pltpu.VMEM)
    hbm = pl.BlockSpec(memory_space=pltpu.HBM)
    dma = pltpu.SemaphoreType.DMA
    near, image = pl.pallas_call(
        functools.partial(kernel, groups, members, specs),
        out_shape=(
            jax.ShapeDtypeStruct((1, colours, rays), f32),
            jax.ShapeDtypeStruct((colours, rays), f32),
        ),
        in_specs=[hbm] * 6,
        out_specs=(vmem, vmem),
        scratch_shapes=[
            pltpu.VMEM(emission.shape, emission.dtype),
            pltpu.VMEM(opacity.shape, opacity.dtype),
            pltpu.VMEM((bins,), f32),
            pltpu.VMEM((rays,), jnp.int32),
            pltpu.VMEM((rays,), jnp.int32),
            pltpu.VMEM((colours, bins), f32),
            pltpu.VMEM((colours, bins, LANES), f32),
            pltpu.VMEM((specs, colours, bins, LANES), f32),
            pltpu.VMEM((tiles, members, bins, LANES), f32),
            pltpu.VMEM((tiles, members, specs, bins, LANES), f32),
            pltpu.VMEM((tiles, members, bins, LANES), f32),
            pltpu.VMEM((tiles, members, specs, bins, LANES), f32),
            pltpu.VMEM((tiles, specs, bins, LANES), f32),
            pltpu.VMEM((tiles, specs, bins, LANES), f32),
            pltpu.VMEM((members, 2, rows * tiles, LANES), f32),
            pltpu.VMEM((members, 2, rows * tiles, LANES), f32),
            pltpu.VMEM((rows * tiles, LANES), f32),
            pltpu.VMEM((groups, members, rows * tiles, LANES), f32),
            dma((tiles,)), dma((tiles,)), dma((4,)), dma, dma((specs,)),
            dma((tiles, members)), dma((tiles, members, specs)),
            dma((tiles, members)), dma((tiles, members, specs)),
            dma((tiles,)), dma((tiles,)),
            dma((members, specs)), dma((members,)),
            dma((max(groups - 1, 1), members, specs)), dma((groups, members)),
            pltpu.SemaphoreType.REGULAR,
        ],
        compiler_params=pltpu.CompilerParams(
            collective_id=0, has_side_effects=True, vmem_limit_bytes=56 * 2**20
        ),
    )(emission, opacity, bin_extinction, entry, exit_cell, response)
    near, image = pl.pallas_call(
        place,
        out_shape=(
            jax.ShapeDtypeStruct((colours, 1, rays), f32),
            jax.ShapeDtypeStruct((colours, rays), f32),
        ),
        in_specs=[vmem, vmem],
        out_specs=(vmem, vmem),
    )(near, image)
    return jnp.transpose(near, (1, 0, 2)), image


def solution(mesh):
    sections = mesh.shape["depth"]
    specs = mesh.shape["spec"]

    def program(emission, *rest):
        rays = emission.shape[2]
        members = max(
            m for m in range(1, sections + 1)
            if sections % m == 0 and rays % (m * LANES) == 0 and (2 * m <= sections or m == 1)
        )
        placed = (
            P("depth", "spec", None),
            P("depth", "spec", None),
            P("spec"),
            P(),
            P(),
            P(None, "spec"),
        )
        return jax.shard_map(
            functools.partial(body, sections // members, members, specs),
            mesh=mesh, in_specs=placed, out_specs=(P("depth", None, None), P()), check_vma=False,
        )(emission, *rest)

    return program
```

```python
import functools
import math
import jax
import jax.numpy as jnp
from jax import lax
from jax.experimental import pallas as pl
from jax.experimental.pallas import tpu as pltpu
from jax.sharding import PartitionSpec as P

LANES = 128
SUBLANES = 8
MESH = pl.DeviceIdType.MESH


def padded(colours):
    return -(-colours // 4) * 4


def column(row, eye):
    return jnp.sum(jnp.where(eye, row, 0.0), axis=1, keepdims=True)


def kernel(
    groups, members, specs,
    em_hbm, op_hbm, ext_hbm, entry_hbm, exit_hbm, resp_hbm,
    near_ref, image_ref,
    em_v, op_v, ext_v, entry_v, exit_v, resp_v, w_own, w_all,
    s_out, s_in, l_out, l_in, d_out, d_in, f_out, f_in, x_out, x_in,
    em_sem, op_sem, piece_sem, small_sem, w_send, w_recv,
    s_send, s_recv, l_send, l_recv, d_send, d_recv, f_send, f_recv, x_send, x_recv, ready,
):
    cells, bins, rays = em_hbm.shape
    colours = resp_hbm.shape[0]
    tiles = rays // (members * LANES)
    half = rays // tiles
    rows = padded(colours)
    sections = groups * members
    cell_step = 1.0 / (cells * sections)
    me = lax.axis_index("depth")
    spec = lax.axis_index("spec")
    g = me // members
    mi = me % members
    lead = specs - 1
    is_lead = spec == lead
    last = members - 1
    paired = members & (members - 1) == 0

    def owner(t):
        if not paired:
            return (mi + 1 + t) % members
        if isinstance(t, int):
            mask = 0 if t == last else (t + 1) // 2 if t % 2 else last - t // 2
        else:
            odd = t % 2
            mask = jnp.where(t == last, 0, odd * ((t + 1) // 2) + (1 - odd) * (last - t // 2))
        who = 0
        bit = 1
        while bit < members:
            who = who + ((mi // bit + mask // bit) % 2) * bit
            bit *= 2
        return who

    def core(group, member, s):
        return (group * members + member, s)

    def lanes(j, q):
        return pl.ds(pl.multiple_of((j * members + q) * LANES, LANES), LANES)

    small = [
        pltpu.make_async_copy(hbm, vmem, small_sem.at[n])
        for n, (hbm, vmem) in enumerate(
            ((entry_hbm, entry_v), (exit_hbm, exit_v), (ext_hbm, ext_v), (resp_hbm, resp_v))
        )
    ]
    for copy in small:
        copy.start()

    def read_piece(t):
        at = lanes(0, owner(t))
        return pltpu.make_async_copy(op_hbm.at[:, :, at], op_v.at[:, :, at], piece_sem.at[t])

    def read(hbm, vmem, sem, j):
        at = pl.ds(j * half, half)
        return pltpu.make_async_copy(hbm.at[:, :, at], vmem.at[:, :, at], sem.at[j])

    for t in range(members):
        read_piece(t).start()
    for j in range(1, tiles):
        read(op_hbm, op_v, op_sem, j).start()

    barrier = pltpu.get_barrier_semaphore()
    near_barrier = groups == 2
    if near_barrier:
        other = 1 - g

        @pl.when(is_lead)
        def _():
            for t in range(members):
                for s in range(specs):
                    if t < last or s != lead:
                        pl.semaphore_signal(
                            barrier, inc=1, device_id=core(g, owner(t), s), device_id_type=MESH
                        )
            pl.semaphore_signal(barrier, inc=1, device_id=core(other, mi, lead), device_id_type=MESH)
    else:
        @pl.loop(1, sections * specs)
        def _(n):
            index = (me * specs + spec + n) % (sections * specs)
            pl.semaphore_signal(
                barrier, inc=1, device_id=(index // specs, index % specs), device_id_type=MESH
            )

    for j in range(tiles):
        read(em_hbm, em_v, em_sem, j).start()

    def enter():
        if near_barrier:
            @pl.when(is_lead)
            def _():
                pl.semaphore_wait(barrier, members)

            @pl.when(spec != lead)
            def _():
                pl.semaphore_wait(barrier, members)
        else:
            pl.semaphore_wait(barrier, sections * specs - 1)

    for copy in small:
        copy.wait()

    eye = lax.broadcasted_iota(jnp.int32, (bins, bins), 0) == lax.broadcasted_iota(
        jnp.int32, (bins, bins), 1
    )
    scale = column(ext_v[...].reshape(1, bins), eye) * (-cell_step * math.log2(math.e))
    scale = jnp.broadcast_to(scale, (bins, LANES))
    for c in range(colours):
        w_own[c] = jnp.broadcast_to(column(resp_v[pl.ds(c, 1), :], eye), (bins, LANES))
    x_out[...] = jnp.zeros_like(x_out)
    f_out[...] = jnp.zeros_like(f_out)
    first = me * cells

    def bounds(at):
        low = jnp.broadcast_to(entry_v[at].reshape(1, LANES) - first, (SUBLANES, LANES))
        high = jnp.broadcast_to(exit_v[at].reshape(1, LANES) - first, (SUBLANES, LANES))
        return low, high

    def live_at(i, low, high):
        return jnp.where((low <= i) & (high > i), 1.0, 0.0)

    def masked(x, live):
        x = x.astype(jnp.float32).reshape(bins // SUBLANES, SUBLANES, LANES)
        return (x * live[None]).reshape(bins, LANES)

    def depth_of(j, t):
        at = lanes(j, owner(t))
        low, high = bounds(at)
        total = jnp.zeros((bins, LANES), jnp.float32)
        for i in range(cells):
            total = total + masked(op_v[i, :, at], live_at(i, low, high))
        s_out[j, t] = total * scale

    def light_of(j, t):
        at = lanes(j, owner(t))
        low, high = bounds(at)
        run = jnp.zeros((bins, LANES), jnp.float32)
        glow = jnp.zeros((bins, LANES), jnp.float32)
        for i in range(cells):
            live = live_at(i, low, high)
            glow = glow + masked(em_v[i, :, at], live) * jnp.exp2(run)
            run = run + masked(op_v[i, :, at], live) * scale
        l_out[j, t] = glow * cell_step

    def piece(out, into, send, recv, j, t):
        return pltpu.make_async_remote_copy(
            out.at[j, t], into.at[j, mi * specs + spec], send, recv.at[j],
            device_id=core(g, owner(t), lead), device_id_type=MESH,
        )

    def leaves(t):
        return (t < last) | (spec != lead)

    depth_args = (s_out, s_in, s_send, s_recv)
    light_args = (l_out, l_in, l_send, l_recv)

    def send(args, j, t):
        @pl.when(leaves(t))
        def _():
            piece(*args, j, t).start()

        @pl.when((t == last) & is_lead)
        def _():
            args[1][j, mi * specs + spec] = args[0][j, t]

    weights_copy = pltpu.make_async_remote_copy(
        w_own, w_all.at[spec], w_send, w_recv, device_id=(me, lead), device_id_type=MESH,
    )

    for j in range(tiles):
        if j > 0:
            read(op_hbm, op_v, op_sem, j).wait()

        @pl.loop(0, members)
        def _(t):
            if j == 0:
                read_piece(t).wait()
            depth_of(j, t)
            if j == 0:
                @pl.when(t == 0)
                def _():
                    enter()
            send(depth_args, j, t)

    @pl.when(is_lead)
    def _():
        w_all[lead] = w_own[...]

    @pl.when(spec != lead)
    def _():
        weights_copy.start()

    for j in range(tiles):
        read(em_hbm, em_v, em_sem, j).wait()

        @pl.loop(0, members)
        def _(t):
            light_of(j, t)
            send(light_args, j, t)

    def landed(ref, recv):
        pltpu.make_async_remote_copy(
            ref, ref, w_send, recv, device_id=(me, lead), device_id_type=MESH
        ).wait_recv()

    def drained(ref, send):
        pltpu.make_async_remote_copy(
            ref, ref, send, w_recv, device_id=(me, lead), device_id_type=MESH
        ).wait_send()

    def arrive(args, j):
        landed(args[1].at[j, pl.ds(0, members * specs - 1)], args[3].at[j])

    def section(ref, j, k):
        return ref[j, pl.ds(k * specs, specs)]

    def chain(j):
        return pltpu.make_async_remote_copy(
            d_out.at[j], d_in.at[j], d_send, d_recv.at[j],
            device_id=core((g + 1) % groups, mi, lead), device_id_type=MESH,
        )

    def total_copy(dg, t, s):
        return pltpu.make_async_remote_copy(
            x_out, x_in.at[dg - 1, mi], x_send.at[dg - 1, s], x_recv.at[dg - 1],
            device_id=core((g + dg) % groups, owner(t), s), device_id_type=MESH,
        )

    def block_copy(t, s):
        k = owner(t)
        return pltpu.make_async_remote_copy(
            f_out.at[k], f_in.at[mi], f_send.at[s], f_recv,
            device_id=core(g, k, s), device_id_type=MESH,
        )

    @pl.when(is_lead)
    def _():
        for j in range(tiles):
            arrive(depth_args, j)

            @pl.when(g == 0)
            def _():
                d_in[j] = jnp.zeros(d_in.shape[1:], jnp.float32)

            if groups > 1:
                @pl.when(g < groups - 1)
                def _():
                    here = section(s_in, j, 0)
                    for k in range(1, members):
                        here = here + section(s_in, j, k)
                    if groups > 2:
                        @pl.when(g > 0)
                        def _():
                            chain(j).wait_recv()

                        here = here + d_in[j]
                    d_out[j] = here
                    chain(j).start()

        if near_barrier:
            @pl.when(g == 1)
            def _():
                pl.semaphore_signal(ready, inc=1, device_id=core(0, mi, lead), device_id_type=MESH)

        if specs > 1:
            landed(w_all.at[pl.ds(0, specs - 1)], w_recv)

        for j in range(tiles):
            arrive(light_args, j)
            if groups > 1:
                @pl.when((g > 0) if groups == 2 else (g == groups - 1))
                def _():
                    chain(j).wait_recv()

            ahead = d_in[j]
            sums = [jnp.zeros((SUBLANES, LANES), jnp.float32) for _ in range(colours)]
            for k in range(members):
                seen = jnp.exp2(ahead) * section(l_in, j, k)
                for c in range(colours):
                    if k > 0:
                        f_out[k, 0, pl.ds(rows * j + c, 1), :] = jnp.sum(sums[c], axis=0, keepdims=True)
                    part = (seen * w_all[:, c]).reshape(-1, SUBLANES, LANES)
                    sums[c] = sums[c] + jnp.sum(part, axis=0)
                if k < members - 1:
                    ahead = ahead + section(s_in, j, k)
            for c in range(colours):
                x_out[pl.ds(rows * j + c, 1), :] = jnp.sum(sums[c], axis=0, keepdims=True)

        if near_barrier:
            @pl.when(g == 0)
            def _():
                pl.semaphore_wait(ready, 1)

        for dg in range(1, groups):
            for t in range(members):
                for s in range(specs):
                    total_copy(dg, t, s).start()
        for k in range(members):
            f_out[k, 1] = x_out[...]
        for t in range(members):
            for s in range(specs):
                if t < last or s != lead:
                    block_copy(t, s).start()
        f_in[mi] = f_out[mi]

    @pl.when(is_lead)
    def _():
        landed(f_in.at[pl.ds(0, last)], f_recv)

    @pl.when(spec != lead)
    def _():
        landed(f_in, f_recv)

    for dg in range(1, groups):
        landed(x_in.at[dg - 1], x_recv.at[dg - 1])

    for q in range(members):
        near = f_in[q, 0]
        image = f_in[q, 1]
        for dg in range(1, groups):
            src = (g + groups - dg) % groups
            value = x_in[dg - 1, q]
            near = near + value * jnp.where(src < g, 1.0, 0.0)
            image = image + value
        for j in range(tiles):
            at = pl.ds((j * members + q) * LANES, LANES)
            near_ref[0, :, at] = near[4 * j:rows * j + colours]
            image_ref[:, at] = image[4 * j:rows * j + colours]
    @pl.when(is_lead)
    def _():
        drained(s_out.at[:, pl.ds(0, last)], s_send)
        drained(l_out.at[:, pl.ds(0, last)], l_send)
        if groups > 1:
            @pl.when(g < groups - 1)
            def _():
                drained(d_out, d_send)
        for s in range(specs):
            drained(f_out.at[pl.ds(0, members if s != lead else last)], f_send.at[s])
        for dg in range(1, groups):
            for s in range(specs):
                drained(x_in.at[dg - 1], x_send.at[dg - 1, s])

    @pl.when(spec != lead)
    def _():
        drained(s_out, s_send)
        drained(l_out, l_send)
        weights_copy.wait_send()


def place(near_ref, image_ref, near_out, image_out):
    for c in range(near_out.shape[0]):
        near_out[c] = near_ref[:, c]
    image_out[...] = image_ref[...]


def body(groups, members, specs, emission, opacity, bin_extinction, entry, exit_cell, response):
    cells, bins, rays = emission.shape
    colours = response.shape[0]
    tiles = rays // (members * LANES)
    rows = padded(colours)
    f32 = jnp.float32
    vmem = pl.BlockSpec(memory_space=pltpu.VMEM)
    hbm = pl.BlockSpec(memory_space=pltpu.HBM)
    dma = pltpu.SemaphoreType.DMA
    near, image = pl.pallas_call(
        functools.partial(kernel, groups, members, specs),
        out_shape=(
            pltpu.VMEM((1, colours, rays), f32),
            pltpu.VMEM((colours, rays), f32),
        ),
        in_specs=[hbm] * 6,
        out_specs=(vmem, vmem),
        scratch_shapes=[
            pltpu.VMEM(emission.shape, emission.dtype),
            pltpu.VMEM(opacity.shape, opacity.dtype),
            pltpu.VMEM((bins,), f32),
            pltpu.VMEM((rays,), jnp.int32),
            pltpu.VMEM((rays,), jnp.int32),
            pltpu.VMEM((colours, bins), f32),
            pltpu.VMEM((colours, bins, LANES), f32),
            pltpu.VMEM((specs, colours, bins, LANES), f32),
            pltpu.VMEM((tiles, members, bins, LANES), f32),
            pltpu.VMEM((tiles, members * specs, bins, LANES), f32),
            pltpu.VMEM((tiles, members, bins, LANES), f32),
            pltpu.VMEM((tiles, members * specs, bins, LANES), f32),
            pltpu.VMEM((tiles, specs, bins, LANES), f32),
            pltpu.VMEM((tiles, specs, bins, LANES), f32),
            pltpu.VMEM((members, 2, rows * tiles, LANES), f32),
            pltpu.VMEM((members, 2, rows * tiles, LANES), f32),
            pltpu.VMEM((rows * tiles, LANES), f32),
            pltpu.VMEM((max(groups - 1, 1), members, rows * tiles, LANES), f32),
            dma((tiles,)), dma((tiles,)), dma((members,)), dma((4,)), dma, dma,
            dma, dma((tiles,)), dma, dma((tiles,)), dma, dma((tiles,)),
            dma((specs,)), dma, dma((max(groups - 1, 1), specs)), dma((max(groups - 1, 1),)),
            pltpu.SemaphoreType.REGULAR,
        ],
        compiler_params=pltpu.CompilerParams(
            collective_id=0, has_side_effects=True, vmem_limit_bytes=56 * 2**20
        ),
    )(emission, opacity, bin_extinction, entry, exit_cell, response)
    near, image = pl.pallas_call(
        place,
        out_shape=(
            jax.ShapeDtypeStruct((colours, 1, rays), f32),
            jax.ShapeDtypeStruct((colours, rays), f32),
        ),
        in_specs=[vmem, vmem],
        out_specs=(vmem, vmem),
    )(*(pltpu.with_memory_space_constraint(x, pltpu.VMEM) for x in (near, image)))
    return jnp.transpose(near, (1, 0, 2)), image


def solution(mesh):
    sections = mesh.shape["depth"]
    specs = mesh.shape["spec"]

    def program(emission, *rest):
        rays = emission.shape[2]
        members = max(
            m for m in range(1, sections + 1)
            if sections % m == 0 and rays % (m * LANES) == 0 and (2 * m <= sections or m == 1)
        )
        placed = (
            P("depth", "spec", None),
            P("depth", "spec", None),
            P("spec"),
            P(),
            P(),
            P(None, "spec"),
        )
        return jax.shard_map(
            functools.partial(body, sections // members, members, specs),
            mesh=mesh, in_specs=placed, out_specs=(P("depth", None, None), P()), check_vma=False,
        )(emission, *rest)

    return program
```

```python
import functools
import math
import jax
import jax.numpy as jnp
from jax import lax
from jax.experimental import pallas as pl
from jax.experimental.pallas import tpu as pltpu
from jax.sharding import PartitionSpec as P

LANES = 128
SUBLANES = 8
MESH = pl.DeviceIdType.MESH


def padded(colours):
    return -(-colours // 4) * 4


def read_runs(count):
    runs = []
    start = 0
    for length in (1, 1, 2, 2, 2, *[4] * count):
        if start < count:
            runs.append((start, min(length, count - start)))
            start += length
    return runs


def column(row, eye):
    return jnp.sum(jnp.where(eye, row, 0.0), axis=1, keepdims=True)


def kernel(
    groups, members, specs,
    em_hbm, op_hbm, ext_hbm, entry_hbm, exit_hbm, resp_hbm,
    near_ref, image_ref,
    data_v, ext_v, entry_v, exit_v, resp_v, w_own, w_all,
    s_out, s_in, l_out, l_in, d_out, d_in, f_out, f_in, x_out, x_in,
    data_sem, small_sem, w_send, w_recv,
    s_send, s_recv, l_send, l_recv, d_send, d_recv, f_send, f_recv, x_send, x_recv, ready,
):
    cells, bins, rays = em_hbm.shape
    colours = resp_hbm.shape[0]
    tiles = rays // (members * LANES)
    rows = padded(colours)
    sections = groups * members
    cell_step = 1.0 / (cells * sections)
    me = lax.axis_index("depth")
    spec = lax.axis_index("spec")
    g = me // members
    mi = me % members
    lead = specs - 1
    is_lead = spec == lead
    last = members - 1
    paired = members & (members - 1) == 0

    def owner(t):
        return mi ^ (last - t) if paired else (mi + 1 + t) % members

    def when(condition, body):
        if condition is True:
            body()
        elif condition is not False:
            pl.when(condition)(body)

    def core(group, member, s):
        return (group * members + member, s)

    def lanes(j, q):
        return pl.ds(pl.multiple_of((j * members + q) * LANES, LANES), LANES)

    count = tiles * members
    ahead_first = (g < groups - 1) if groups > 1 and count % 2 == 0 else False

    def place_of(p):
        return p // members, p % members

    def read(n, hbm, p, sem):
        j, t = place_of(p)
        at = lanes(j, owner(t))
        return pltpu.make_async_copy(hbm.at[:, :, at], data_v.at[n, :, :, at], data_sem.at[sem])

    runs = read_runs(count)

    def sem_of(pair):
        return next(n for n, (start, length) in enumerate(runs) if start <= pair < start + length)

    def read_wait(number, extra=True):
        for n, (start, length) in enumerate(runs):
            def wait():
                pairs = data_v.at[:, :, :, pl.ds(0, length * LANES)]
                pltpu.make_async_copy(pairs, pairs, data_sem.at[n]).wait()

            when((number == start) if extra is True else extra & (number == start), wait)

    together = jnp.logical_not(ahead_first) if ahead_first is not False else True

    first_read = read(0, op_hbm, 0, 0)
    first_read.start()

    small = [
        pltpu.make_async_copy(hbm, vmem, small_sem.at[n])
        for n, (hbm, vmem) in enumerate(
            ((entry_hbm, entry_v), (exit_hbm, exit_v), (ext_hbm, ext_v), (resp_hbm, resp_v))
        )
    ]
    for copy in small:
        copy.start()

    barrier = pltpu.get_barrier_semaphore()
    near_barrier = groups == 2

    def greet(group, member, s):
        pl.semaphore_signal(barrier, inc=1, device_id=core(group, member, s), device_id_type=MESH)

    if near_barrier:
        @pl.when(is_lead)
        def _():
            for s in range(specs - 1):
                greet(g, mi, s)

    def read_in_turn():
        for p in range(1, count):
            read(0, op_hbm, p, sem_of(p // 2)).start()
        for p in range(count):
            read(1, em_hbm, p, sem_of((count + p) // 2)).start()

    def read_together():
        for p in range(count):
            if p > 0:
                read(0, op_hbm, p, sem_of(p)).start()
            read(1, em_hbm, p, sem_of(p)).start()

    when(ahead_first, read_in_turn)
    when(together, read_together)

    if near_barrier:
        @pl.when(is_lead)
        def _():
            for t in range(last):
                for s in range(specs):
                    greet(g, owner(t), s)


            @pl.when(g == 0)
            def _():
                greet(1, mi, lead)
    else:
        @pl.loop(1, sections * specs)
        def _(n):
            index = (me * specs + spec + n) % (sections * specs)
            greet(index // (members * specs), index // specs % members, index % specs)

    def answer():
        pl.semaphore_signal(ready, inc=1, device_id=core(0, mi, lead), device_id_type=MESH)

    def enter():
        if near_barrier:
            @pl.when(is_lead & (g == 0))
            def _():
                if last > 0:
                    pl.semaphore_wait(barrier, last)

            @pl.when(is_lead & (g == 1))
            def _():
                pl.semaphore_wait(barrier, members)
                answer()

            @pl.when(spec != lead)
            def _():
                pl.semaphore_wait(barrier, members)
        else:
            pl.semaphore_wait(barrier, sections * specs - 1)

    for copy in small[:3]:
        copy.wait()

    eye = lax.broadcasted_iota(jnp.int32, (bins, bins), 0) == lax.broadcasted_iota(
        jnp.int32, (bins, bins), 1
    )
    scale = column(ext_v[...].reshape(1, bins), eye) * (-cell_step * math.log2(math.e))
    scale = jnp.broadcast_to(scale, (bins, LANES))
    scale = scale.reshape(-1, SUBLANES, LANES)
    first = me * cells

    def bounds(at):
        low = jnp.broadcast_to(entry_v[at].reshape(1, LANES) - first, (SUBLANES, LANES))
        high = jnp.broadcast_to(exit_v[at].reshape(1, LANES) - first, (SUBLANES, LANES))
        return low, high

    def march(j, t, slot, entering, leaving):
        at = lanes(j, owner(t))
        low, high = bounds(at)
        run = jnp.zeros_like(scale)
        glow = jnp.zeros_like(scale)
        for i in range(cells):
            dense = data_v[0, i, :, at].astype(jnp.float32).reshape(scale.shape)
            shine = data_v[1, i, :, at].astype(jnp.float32).reshape(scale.shape)
            if entering:
                entered = jnp.where(low <= i, 1.0, 0.0)
                dense = dense * entered[None]
            if entering and leaving:
                shine = shine * jnp.where(high > i, entered, 0.0)[None]
            elif entering:
                shine = shine * entered[None]
            elif leaving:
                shine = shine * jnp.where(high > i, 1.0, 0.0)[None]
            glow = glow + shine * jnp.exp2(run)
            run = run + dense * scale
        s_out[slot] = run.reshape(bins, LANES)
        l_out[j * members + t] = (glow * cell_step).reshape(bins, LANES)

    def march_here(j, t, slot):
        if sections % 4:
            march(j, t, slot, True, True)
            return

        @pl.when(4 * me < sections)
        def _():
            march(j, t, slot, True, False)

        @pl.when((4 * me >= sections) & (4 * me < 3 * sections))
        def _():
            march(j, t, slot, False, False)

        @pl.when(4 * me >= 3 * sections)
        def _():
            march(j, t, slot, False, True)

    def depth_of(j, t, entering):
        at = lanes(j, owner(t))
        low, _ = bounds(at)
        total = jnp.zeros_like(scale)
        for i in range(cells):
            dense = data_v[0, i, :, at].astype(jnp.float32).reshape(scale.shape)
            if entering:
                dense = dense * jnp.where(low <= i, 1.0, 0.0)[None]
            total = total + dense
        s_out[j * members + t] = (total * scale).reshape(bins, LANES)

    def depth_here(j, t):
        if sections % 4:
            depth_of(j, t, True)
            return

        @pl.when(4 * me < sections)
        def _():
            depth_of(j, t, True)

        @pl.when(4 * me >= sections)
        def _():
            depth_of(j, t, False)

    def piece(out, into, send, recv, j, t):
        return pltpu.make_async_remote_copy(
            out.at[j * members + t], into.at[j, mi * specs + spec], send, recv.at[j],
            device_id=core(g, owner(t), lead), device_id_type=MESH,
        )

    def needed(j):
        return (g < groups - 1) | (mi < last) | (j == 0)

    def leaves(t):
        return (t < last) | (spec != lead)

    depth_args = (s_out, s_in, s_send, s_recv)
    light_args = (l_out, l_in, l_send, l_recv)

    def send(args, j, t):
        @pl.when(leaves(t))
        def _():
            piece(*args, j, t).start()

        @pl.when((t == last) & is_lead)
        def _():
            args[1][j, mi * specs + spec] = args[0][j * members + t]

    weights_copy = pltpu.make_async_remote_copy(
        w_own, w_all.at[spec], w_send, w_recv, device_id=(me, lead), device_id_type=MESH,
    )

    def landed(ref, recv):
        pltpu.make_async_remote_copy(
            ref, ref, w_send, recv, device_id=(me, lead), device_id_type=MESH
        ).wait_recv()

    def drained(ref, send):
        pltpu.make_async_remote_copy(
            ref, ref, send, w_recv, device_id=(me, lead), device_id_type=MESH
        ).wait_send()

    def depth_sent():
        @pl.when(is_lead)
        def _():
            drained(s_out.at[pl.ds(0, tiles * last)], s_send)

        @pl.when(spec != lead)
        def _():
            drained(s_out.at[pl.ds(0, count)], s_send)

    def first_pass():
        hold = jnp.minimum(count - 1, 4 + 2 * (last - mi))

        @pl.loop(0, count)
        def _(p):
            j, t = place_of(p)

            read_wait(p // 2, p % 2 == 0)
            depth_here(j, t)

            @pl.when(p == hold)
            def _():
                enter()

                @pl.loop(0, hold)
                def _(u):
                    send(depth_args, *place_of(u))

            @pl.when(p >= hold)
            def _():
                send(depth_args, j, t)

    when(ahead_first, first_pass)

    def second_pass():
        hold = 2 * (last - mi) // 3
        if ahead_first is not False:
            hold = jnp.where(ahead_first, count * 3 // 8, hold)

        def leave(u):
            j, t = place_of(u)

            def depth():
                send(depth_args, j, t)

            when(needed(j) if together is True else together & needed(j), depth)
            send(light_args, j, t)

        @pl.loop(0, count)
        def _(p):
            if ahead_first is False:
                read_wait(p)
                slot = p
            else:
                read_wait(jnp.where(together, p, (count + p) // 2), together | (p % 2 == 0))
                slot = jnp.where(together, p, count)
            march_here(*place_of(p), slot)

            @pl.when(p == hold)
            def _():
                when(together, enter)
                when(ahead_first, depth_sent)

                @pl.loop(0, hold)
                def _(u):
                    leave(u)

            @pl.when(p >= hold)
            def _():
                leave(p)

    second_pass()

    small[3].wait()
    for c in range(colours):
        w_own[c] = jnp.broadcast_to(column(resp_v[pl.ds(c, 1), :], eye), (bins, LANES))
    x_out[...] = jnp.zeros_like(x_out)
    f_out[...] = jnp.zeros_like(f_out)

    @pl.when(is_lead)
    def _():
        w_all[lead] = w_own[...]

    @pl.when(spec != lead)
    def _():
        weights_copy.start()

    def arrive(args, j):
        landed(args[1].at[j, pl.ds(0, members * specs - 1)], args[3].at[j])

    def arrive_depth(j):
        if j == 0:
            arrive(depth_args, j)
            return

        @pl.when(g < groups - 1)
        def _():
            arrive(depth_args, j)

        @pl.when((g == groups - 1) & (mi < last))
        def _():
            if last > 0:
                landed(s_in.at[j, pl.ds(0, last * specs - 1)], s_recv.at[j])

        @pl.when((g == groups - 1) & (mi == last))
        def _():
            if last > 0:
                landed(s_in.at[j, pl.ds(0, last * specs)], s_recv.at[j])

    def section(ref, j, k):
        return ref[j, pl.ds(k * specs, specs)]

    def chain_start(j):
        for s in range(specs):
            for v in range(0, bins, SUBLANES):
                at = (j, s, pl.ds(v, SUBLANES))
                pltpu.make_async_remote_copy(
                    d_out.at[at], d_in.at[at], d_send, d_recv.at[j],
                    device_id=core((g + 1) % groups, mi, lead), device_id_type=MESH,
                ).start()

    def chain_wait(j):
        landed(d_in.at[j], d_recv.at[j])

    def total_copy(dg, k, s):
        return pltpu.make_async_remote_copy(
            x_out, x_in.at[dg - 1, mi], x_send.at[dg - 1, s], x_recv.at[dg - 1],
            device_id=core((g + dg) % groups, k, s), device_id_type=MESH,
        )

    def block_copy(k, s):
        return pltpu.make_async_remote_copy(
            f_out.at[k], f_in.at[mi], f_send.at[s], f_recv,
            device_id=core(g, k, s), device_id_type=MESH,
        )

    @pl.when(is_lead)
    def _():
        for j in range(tiles):
            arrive_depth(j)

            if near_barrier and j == 0:
                @pl.when(g == 1)
                def _():
                    answer()

            @pl.when(g == 0)
            def _():
                d_in[j] = jnp.zeros(d_in.shape[1:], jnp.float32)

            if groups > 1:
                @pl.when(g < groups - 1)
                def _():
                    here = section(s_in, j, 0)
                    for k in range(1, members):
                        here = here + section(s_in, j, k)
                    if groups > 2:
                        @pl.when(g > 0)
                        def _():
                            chain_wait(j)

                        here = here + d_in[j]
                    d_out[j] = here
                    if near_barrier and j == 0:
                        pl.semaphore_wait(ready, 1)
                    chain_start(j)

        if specs > 1:
            landed(w_all.at[pl.ds(0, specs - 1)], w_recv)

        for j in range(tiles):
            arrive(light_args, j)
            if groups > 1:
                @pl.when((g > 0) if groups == 2 else (g == groups - 1))
                def _():
                    chain_wait(j)

            ahead = d_in[j]
            sums = [jnp.zeros((SUBLANES, LANES), jnp.float32) for _ in range(colours)]
            for k in range(members):
                seen = jnp.exp2(ahead) * section(l_in, j, k)
                for c in range(colours):
                    if k > 0:
                        f_out[k, 0, pl.ds(rows * j + c, 1), :] = jnp.sum(sums[c], axis=0, keepdims=True)
                    part = (seen * w_all[:, c]).reshape(-1, SUBLANES, LANES)
                    sums[c] = sums[c] + jnp.sum(part, axis=0)
                if k < members - 1:
                    ahead = ahead + section(s_in, j, k)
            for c in range(colours):
                x_out[pl.ds(rows * j + c, 1), :] = jnp.sum(sums[c], axis=0, keepdims=True)

        if near_barrier:
            @pl.when(g == 0)
            def _():
                pl.semaphore_wait(ready, 1)

        for k in range(members):
            for dg in range(1, groups):
                for s in range(specs):
                    total_copy(dg, k, s).start()
        for k in range(members):
            f_out[k, 1] = x_out[...]
        for k in range(members):
            for s in range(specs):
                @pl.when((k != mi) | (s != lead))
                def _():
                    block_copy(k, s).start()
        f_in[mi] = f_out[mi]

    @pl.when(is_lead)
    def _():
        landed(f_in.at[pl.ds(0, last)], f_recv)

    @pl.when(spec != lead)
    def _():
        landed(f_in, f_recv)

    for dg in range(1, groups):
        landed(x_in.at[dg - 1], x_recv.at[dg - 1])

    for q in range(members):
        near = f_in[q, 0]
        image = f_in[q, 1]
        for dg in range(1, groups):
            src = (g + groups - dg) % groups
            value = x_in[dg - 1, q]
            near = near + value * jnp.where(src < g, 1.0, 0.0)
            image = image + value
        for j in range(tiles):
            at = pl.ds((j * members + q) * LANES, LANES)
            near_ref[0, :, at] = near[rows * j:rows * j + colours]
            image_ref[:, at] = image[rows * j:rows * j + colours]
    when((mi < last) if together is True else together & (mi < last), depth_sent)

    @pl.when((g == groups - 1) & (mi == last))
    def _():
        @pl.when(is_lead)
        def _():
            if last > 0:
                drained(s_out.at[pl.ds(0, last)], s_send)

        @pl.when(spec != lead)
        def _():
            drained(s_out.at[pl.ds(0, members)], s_send)

    @pl.when(is_lead)
    def _():
        drained(l_out.at[pl.ds(0, tiles * last)], l_send)
        if groups > 1:
            @pl.when(g < groups - 1)
            def _():
                drained(d_out, d_send)
        for s in range(specs):
            drained(f_out.at[pl.ds(0, members if s != lead else last)], f_send.at[s])
        for dg in range(1, groups):
            for s in range(specs):
                drained(x_in.at[dg - 1], x_send.at[dg - 1, s])

    @pl.when(spec != lead)
    def _():
        drained(l_out, l_send)
        weights_copy.wait_send()


def place(near_ref, image_ref, near_out, image_out):
    for c in range(near_out.shape[0]):
        near_out[c] = near_ref[:, c]
    image_out[...] = image_ref[...]


def body(groups, members, specs, emission, opacity, bin_extinction, entry, exit_cell, response):
    cells, bins, rays = emission.shape
    colours = response.shape[0]
    tiles = rays // (members * LANES)
    rows = padded(colours)
    f32 = jnp.float32
    vmem = pl.BlockSpec(memory_space=pltpu.VMEM)
    hbm = pl.BlockSpec(memory_space=pltpu.HBM)
    dma = pltpu.SemaphoreType.DMA
    near, image = pl.pallas_call(
        functools.partial(kernel, groups, members, specs),
        out_shape=(
            pltpu.VMEM((1, colours, rays), f32),
            pltpu.VMEM((colours, rays), f32),
        ),
        in_specs=[hbm] * 6,
        out_specs=(vmem, vmem),
        scratch_shapes=[
            pltpu.VMEM((2, *emission.shape), emission.dtype),
            pltpu.VMEM((bins,), f32),
            pltpu.VMEM((rays,), jnp.int32),
            pltpu.VMEM((rays,), jnp.int32),
            pltpu.VMEM((colours, bins), f32),
            pltpu.VMEM((colours, bins, LANES), f32),
            pltpu.VMEM((specs, colours, bins, LANES), f32),
            pltpu.VMEM((tiles * members + 1, bins, LANES), f32),
            pltpu.VMEM((tiles, members * specs, bins, LANES), f32),
            pltpu.VMEM((tiles * members, bins, LANES), f32),
            pltpu.VMEM((tiles, members * specs, bins, LANES), f32),
            pltpu.VMEM((tiles, specs, bins, LANES), f32),
            pltpu.VMEM((tiles, specs, bins, LANES), f32),
            pltpu.VMEM((members, 2, rows * tiles, LANES), f32),
            pltpu.VMEM((members, 2, rows * tiles, LANES), f32),
            pltpu.VMEM((rows * tiles, LANES), f32),
            pltpu.VMEM((max(groups - 1, 1), members, rows * tiles, LANES), f32),
            dma((len(read_runs(tiles * members)),)), dma((4,)), dma, dma,
            dma, dma((tiles,)), dma, dma((tiles,)), dma, dma((tiles,)),
            dma((specs,)), dma, dma((max(groups - 1, 1), specs)), dma((max(groups - 1, 1),)),
            pltpu.SemaphoreType.REGULAR,
        ],
        compiler_params=pltpu.CompilerParams(
            collective_id=0, has_side_effects=True, vmem_limit_bytes=56 * 2**20,
        ),
    )(emission, opacity, bin_extinction, entry, exit_cell, response)
    near, image = pl.pallas_call(
        place,
        out_shape=(
            jax.ShapeDtypeStruct((colours, 1, rays), f32),
            jax.ShapeDtypeStruct((colours, rays), f32),
        ),
        in_specs=[vmem, vmem],
        out_specs=(vmem, vmem),
    )(*(pltpu.with_memory_space_constraint(x, pltpu.VMEM) for x in (near, image)))
    return jnp.transpose(near, (1, 0, 2)), image


def solution(mesh):
    sections = mesh.shape["depth"]
    specs = mesh.shape["spec"]

    def program(emission, *rest):
        rays = emission.shape[2]
        members = max(
            m for m in range(1, sections + 1)
            if sections % m == 0 and rays % (m * LANES) == 0 and (2 * m <= sections or m == 1)
        )
        placed = (
            P("depth", "spec", None),
            P("depth", "spec", None),
            P("spec"),
            P(),
            P(),
            P(None, "spec"),
        )
        return jax.shard_map(
            functools.partial(body, sections // members, members, specs),
            mesh=mesh, in_specs=placed, out_specs=(P("depth", None, None), P()), check_vma=False,
        )(emission, *rest)

    return program
```

```python
import functools
import math
import jax
import jax.numpy as jnp
from jax import lax
from jax.experimental import pallas as pl
from jax.experimental.pallas import tpu as pltpu
from jax.sharding import PartitionSpec as P

LANES = 128
SUBLANES = 8
MESH = pl.DeviceIdType.MESH


def padded(colours):
    return -(-colours // 4) * 4


def read_runs(count):
    runs = []
    start = 0
    for length in (1, 1, 2, 4, *[8] * count):
        if start < count:
            runs.append((start, min(length, count - start)))
            start += length
    return runs


def column(row, eye):
    return jnp.sum(jnp.where(eye, row, 0.0), axis=1, keepdims=True)


def kernel(
    groups, members, specs,
    em_hbm, op_hbm, ext_hbm, entry_hbm, exit_hbm, resp_hbm,
    near_ref, image_ref,
    data_v, scale_v, ext_v, bounds_v, resp_v, w_own, w_all,
    s_out, s_in, l_out, l_in, d_out, d_in, f_out, f_in, x_out, x_in, shape_v,
    data_sem, small_sem, w_send, w_recv,
    s_send, s_recv, l_send, l_recv, d_send, d_recv, f_send, f_recv, x_send, x_recv, ready,
):
    cells, bins, rays = em_hbm.shape
    colours = resp_hbm.shape[0]
    tiles = rays // (members * LANES)
    rows = padded(colours)
    sections = groups * members
    cell_step = 1.0 / (cells * sections)
    me = lax.axis_index("depth")
    spec = lax.axis_index("spec")
    g = me // members
    mi = me % members
    lead = specs - 1
    is_lead = spec == lead
    last = members - 1
    paired = members & (members - 1) == 0

    def owner(t):
        return mi ^ (last - t) if paired else (mi + 1 + t) % members

    def when(condition, body):
        if condition is True:
            body()
        elif condition is not False:
            pl.when(condition)(body)

    def core(group, member, s):
        return (group * members + member, s)

    def lanes(j, q):
        return pl.ds(pl.multiple_of((j * members + q) * LANES, LANES), LANES)

    count = tiles * members
    ahead_first = (g < groups - 1) if groups > 1 and count % 2 == 0 else False

    def place_of(p):
        return p // members, p % members

    def read(n, hbm, p, sem):
        j, t = place_of(p)
        at = lanes(j, owner(t))
        return pltpu.make_async_copy(
            hbm.at[:, :, at], data_v.at[n, j * members + t], data_sem.at[sem]
        )

    runs = read_runs(count)

    def sem_of(pair):
        return next(n for n, (start, length) in enumerate(runs) if start <= pair < start + length)

    def read_wait(number, extra=True):
        for n, (start, length) in enumerate(runs):
            def wait():
                pairs = data_v.at[:, pl.ds(0, length)]
                pltpu.make_async_copy(pairs, pairs, data_sem.at[n]).wait()

            when((number == start) if extra is True else extra & (number == start), wait)

    together = jnp.logical_not(ahead_first) if ahead_first is not False else True

    first_read = read(0, op_hbm, 0, 0)
    first_read.start()

    small = [
        pltpu.make_async_copy(hbm, vmem, small_sem.at[n])
        for n, (hbm, vmem) in enumerate(
            ((ext_hbm, ext_v), (resp_hbm, resp_v))
        )
    ]
    for n, hbm in enumerate((entry_hbm, exit_hbm)):
        pltpu.make_async_copy(hbm, bounds_v.at[pl.ds(n * rays, rays)], small_sem.at[2]).start()
    for copy in small:
        copy.start()

    barrier = pltpu.get_barrier_semaphore()
    near_barrier = groups == 2

    def greet(group, member, s):
        pl.semaphore_signal(barrier, inc=1, device_id=core(group, member, s), device_id_type=MESH)

    if near_barrier:
        @pl.when(is_lead)
        def _():
            for s in range(specs - 1):
                greet(g, mi, s)

    def read_in_turn():
        for p in range(1, count):
            read(0, op_hbm, p, sem_of(p // 2)).start()
        for p in range(count):
            read(1, em_hbm, p, sem_of((count + p) // 2)).start()

    def read_together():
        for p in range(count):
            if p > 0:
                read(0, op_hbm, p, sem_of(p)).start()
            read(1, em_hbm, p, sem_of(p)).start()

    when(ahead_first, read_in_turn)
    when(together, read_together)

    if near_barrier:
        @pl.when(is_lead)
        def _():
            for t in range(last):
                for s in range(specs):
                    greet(g, owner(t), s)


            @pl.when(g == 0)
            def _():
                greet(1, mi, lead)
    else:
        @pl.loop(1, sections * specs)
        def _(n):
            index = (me * specs + spec + n) % (sections * specs)
            greet(index // (members * specs), index // specs % members, index % specs)

    def answer():
        pl.semaphore_signal(ready, inc=1, device_id=core(0, mi, lead), device_id_type=MESH)

    def enter():
        if near_barrier:
            @pl.when(is_lead & (g == 0))
            def _():
                if last > 0:
                    pl.semaphore_wait(barrier, last)

            @pl.when(is_lead & (g == 1))
            def _():
                pl.semaphore_wait(barrier, members)
                answer()

            @pl.when(spec != lead)
            def _():
                pl.semaphore_wait(barrier, members)
        else:
            pl.semaphore_wait(barrier, sections * specs - 1)

    pltpu.make_async_copy(bounds_v, bounds_v, small_sem.at[2]).wait()
    small[0].wait()

    eye = lax.broadcasted_iota(jnp.int32, (bins, bins), 0) == lax.broadcasted_iota(
        jnp.int32, (bins, bins), 1
    )
    scale = column(ext_v[...].reshape(1, bins), eye) * (-cell_step * math.log2(math.e))
    scale = jnp.broadcast_to(scale, (bins, LANES))
    scale_v[...] = scale.reshape(-1, SUBLANES, LANES)
    first = me * cells

    def bounds(j, t):
        at = (j * members + owner(t)) * LANES
        low = bounds_v[pl.ds(pl.multiple_of(at, LANES), LANES)].reshape(1, LANES) - first
        high = bounds_v[pl.ds(pl.multiple_of(rays + at, LANES), LANES)].reshape(1, LANES) - first
        low = jnp.broadcast_to(low, (SUBLANES, LANES))
        high = jnp.broadcast_to(high, (SUBLANES, LANES))
        return low, high

    def march(j, t, slot, entering, leaving):
        low, high = bounds(j, t)
        run = jnp.zeros(scale_v.shape, jnp.float32)
        glow = jnp.zeros(scale_v.shape, jnp.float32)
        for i in range(cells):
            dense = data_v[0, j * members + t, i].astype(jnp.float32).reshape(scale_v.shape)
            shine = data_v[1, j * members + t, i].astype(jnp.float32).reshape(scale_v.shape)
            if entering:
                entered = jnp.where(low <= i, 1.0, 0.0)
                dense = dense * entered[None]
            if entering and leaving:
                shine = shine * jnp.where(high > i, entered, 0.0)[None]
            elif entering:
                shine = shine * entered[None]
            elif leaving:
                shine = shine * jnp.where(high > i, 1.0, 0.0)[None]
            glow = glow + shine * jnp.exp2(run)
            run = run + dense * scale_v[...]
        s_out[slot] = run.reshape(bins, LANES)
        l_out[j * members + t] = (glow * cell_step).reshape(bins, LANES)

    def march_here(j, t, slot):
        if sections % 4:
            march(j, t, slot, True, True)
            return

        @pl.when(4 * me < sections)
        def _():
            march(j, t, slot, True, False)

        @pl.when((4 * me >= sections) & (4 * me < 3 * sections))
        def _():
            march(j, t, slot, False, False)

        @pl.when(4 * me >= 3 * sections)
        def _():
            march(j, t, slot, False, True)

    def depth_of(j, t, entering):
        low, _ = bounds(j, t)
        total = jnp.zeros(scale_v.shape, jnp.float32)
        for i in range(cells):
            dense = data_v[0, j * members + t, i].astype(jnp.float32).reshape(scale_v.shape)
            if entering:
                dense = dense * jnp.where(low <= i, 1.0, 0.0)[None]
            total = total + dense
        s_out[j * members + t] = (total * scale_v[...]).reshape(bins, LANES)

    def depth_here(j, t):
        if sections % 4:
            depth_of(j, t, True)
            return

        @pl.when(4 * me < sections)
        def _():
            depth_of(j, t, True)

        @pl.when(4 * me >= sections)
        def _():
            depth_of(j, t, False)

    def piece(out, into, send, recv, j, t):
        return pltpu.make_async_remote_copy(
            out.at[j * members + t], into.at[j, mi * specs + spec], send, recv.at[j],
            device_id=core(g, owner(t), lead), device_id_type=MESH,
        )

    def needed(j):
        return (g < groups - 1) | (mi < last) | (j == 0)

    def leaves(t):
        return (t < last) | (spec != lead)

    depth_args = (s_out, s_in, s_send, s_recv)
    light_args = (l_out, l_in, l_send, l_recv)

    def send(args, j, t):
        @pl.when(leaves(t))
        def _():
            piece(*args, j, t).start()

        @pl.when((t == last) & is_lead)
        def _():
            args[1][j, mi * specs + spec] = args[0][j * members + t]

    weights_copy = pltpu.make_async_remote_copy(
        w_own, w_all.at[spec], w_send, w_recv, device_id=(me, lead), device_id_type=MESH,
    )

    def landed(ref, recv):
        pltpu.make_async_remote_copy(
            ref, ref, w_send, recv, device_id=(me, lead), device_id_type=MESH
        ).wait_recv()

    def drained(ref, send):
        pltpu.make_async_remote_copy(
            ref, ref, send, w_recv, device_id=(me, lead), device_id_type=MESH
        ).wait_send()

    def depth_sent():
        @pl.when(is_lead)
        def _():
            drained(s_out.at[pl.ds(0, tiles * last)], s_send)

        @pl.when(spec != lead)
        def _():
            drained(s_out.at[pl.ds(0, count)], s_send)

    def first_pass():
        hold = jnp.minimum(count - 1, 4 + 2 * (last - mi))

        @pl.loop(0, count)
        def _(p):
            j, t = place_of(p)

            read_wait(p // 2, p % 2 == 0)
            depth_here(j, t)

            @pl.when(p == hold)
            def _():
                enter()

                @pl.loop(0, hold)
                def _(u):
                    send(depth_args, *place_of(u))

            @pl.when(p >= hold)
            def _():
                send(depth_args, j, t)

    when(ahead_first, first_pass)

    def second_pass():
        hold = 0 if ahead_first is False else jnp.where(ahead_first, count * 3 // 8, 0)

        def leave(u):
            j, t = place_of(u)

            def depth():
                send(depth_args, j, t)

            when(needed(j) if together is True else together & needed(j), depth)
            send(light_args, j, t)

        @pl.loop(0, count)
        def _(p):
            if ahead_first is False:
                read_wait(p)
                slot = p
            else:
                read_wait(jnp.where(together, p, (count + p) // 2), together | (p % 2 == 0))
                slot = jnp.where(together, p, count)
            march_here(*place_of(p), slot)

            @pl.when(p == hold)
            def _():
                when(together, enter)
                when(ahead_first, depth_sent)

                @pl.loop(0, hold)
                def _(u):
                    leave(u)

            @pl.when(p >= hold)
            def _():
                leave(p)

    second_pass()

    small[1].wait()
    for c in range(colours):
        w_own[c] = jnp.broadcast_to(column(resp_v[pl.ds(c, 1), :], eye), (bins, LANES))
    x_out[...] = jnp.zeros_like(x_out)
    f_out[...] = jnp.zeros_like(f_out)

    @pl.when(is_lead)
    def _():
        w_all[lead] = w_own[...]

    @pl.when(spec != lead)
    def _():
        weights_copy.start()

    def arrive(args, j):
        landed(args[1].at[j, pl.ds(0, members * specs - 1)], args[3].at[j])

    def arrive_depth(j):
        if j == 0:
            arrive(depth_args, j)
            return

        @pl.when(g < groups - 1)
        def _():
            arrive(depth_args, j)

        @pl.when((g == groups - 1) & (mi < last))
        def _():
            if last > 0:
                landed(s_in.at[j, pl.ds(0, last * specs - 1)], s_recv.at[j])

        @pl.when((g == groups - 1) & (mi == last))
        def _():
            if last > 0:
                landed(s_in.at[j, pl.ds(0, last * specs)], s_recv.at[j])

    def section(ref, j, k):
        return ref[j, pl.ds(k * specs, specs)]

    def chain_start(j):
        for s in range(specs):
            for v in range(0, bins, SUBLANES):
                at = (j, s, pl.ds(v, SUBLANES))
                pltpu.make_async_remote_copy(
                    d_out.at[at], d_in.at[at], d_send, d_recv.at[j],
                    device_id=core((g + 1) % groups, mi, lead), device_id_type=MESH,
                ).start()

    def chain_wait(j):
        landed(d_in.at[j], d_recv.at[j])

    def total_copy(dg, k, s):
        return pltpu.make_async_remote_copy(
            x_out, x_in.at[dg - 1, mi], x_send.at[dg - 1], x_recv.at[dg - 1],
            device_id=core((g + dg) % groups, k, s), device_id_type=MESH,
        )

    def block_copy(k, s):
        return pltpu.make_async_remote_copy(
            f_out.at[k], f_in.at[mi], f_send, f_recv,
            device_id=core(g, k, s), device_id_type=MESH,
        )

    @pl.when(is_lead)
    def _():
        for j in range(tiles):
            arrive_depth(j)

            if near_barrier and j == 0:
                @pl.when(g == 1)
                def _():
                    answer()

            @pl.when(g == 0)
            def _():
                d_in[j] = jnp.zeros(d_in.shape[1:], jnp.float32)

            if groups > 1:
                @pl.when(g < groups - 1)
                def _():
                    here = section(s_in, j, 0)
                    for k in range(1, members):
                        here = here + section(s_in, j, k)
                    if groups > 2:
                        @pl.when(g > 0)
                        def _():
                            chain_wait(j)

                        here = here + d_in[j]
                    d_out[j] = here
                    if near_barrier and j == 0:
                        pl.semaphore_wait(ready, 1)
                    chain_start(j)

        if specs > 1:
            landed(w_all.at[pl.ds(0, specs - 1)], w_recv)

        for j in range(tiles):
            arrive(light_args, j)
            if groups > 1:
                @pl.when((g > 0) if groups == 2 else (g == groups - 1))
                def _():
                    chain_wait(j)

            ahead = d_in[j]
            sums = [jnp.zeros((SUBLANES, LANES), jnp.float32) for _ in range(colours)]
            for k in range(members):
                seen = jnp.exp2(ahead) * section(l_in, j, k)
                for c in range(colours):
                    if k > 0:
                        f_out[k, 0, pl.ds(rows * j + c, 1), :] = jnp.sum(sums[c], axis=0, keepdims=True)
                    part = (seen * w_all[:, c]).reshape(-1, SUBLANES, LANES)
                    sums[c] = sums[c] + jnp.sum(part, axis=0)
                if k < members - 1:
                    ahead = ahead + section(s_in, j, k)
            for c in range(colours):
                x_out[pl.ds(rows * j + c, 1), :] = jnp.sum(sums[c], axis=0, keepdims=True)

        if near_barrier:
            @pl.when(g == 0)
            def _():
                pl.semaphore_wait(ready, 1)

        for k in range(members):
            for dg in range(1, groups):
                for s in range(specs):
                    total_copy(dg, k, s).start()
        for k in range(members):
            f_out[k, 1] = x_out[...]
        for k in range(members):
            for s in range(specs):
                @pl.when((k != mi) | (s != lead))
                def _():
                    block_copy(k, s).start()
        f_in[mi] = f_out[mi]

    @pl.when(is_lead)
    def _():
        landed(f_in.at[pl.ds(0, last)], f_recv)

    @pl.when(spec != lead)
    def _():
        landed(f_in, f_recv)

    for dg in range(1, groups):
        landed(x_in.at[dg - 1], x_recv.at[dg - 1])

    for q in range(members):
        near = f_in[q, 0]
        image = f_in[q, 1]
        for dg in range(1, groups):
            src = (g + groups - dg) % groups
            value = x_in[dg - 1, q]
            near = near + value * jnp.where(src < g, 1.0, 0.0)
            image = image + value
        for j in range(tiles):
            at = pl.ds((j * members + q) * LANES, LANES)
            near_ref[0, :, at] = near[rows * j:rows * j + colours]
            image_ref[:, at] = image[rows * j:rows * j + colours]
    when((mi < last) if together is True else together & (mi < last), depth_sent)

    @pl.when((g == groups - 1) & (mi == last))
    def _():
        @pl.when(is_lead)
        def _():
            if last > 0:
                drained(s_out.at[pl.ds(0, last)], s_send)

        @pl.when(spec != lead)
        def _():
            drained(s_out.at[pl.ds(0, members)], s_send)

    @pl.when(is_lead)
    def _():
        drained(l_out.at[pl.ds(0, tiles * last)], l_send)
        if groups > 1:
            @pl.when(g < groups - 1)
            def _():
                drained(d_out, d_send)
        drained(shape_v.at[pl.ds(0, members * specs - 1)], f_send)
        for dg in range(1, groups):
            drained(shape_v.at[:, 0], x_send.at[dg - 1])

    @pl.when(spec != lead)
    def _():
        drained(l_out, l_send)
        weights_copy.wait_send()


def place(near_ref, image_ref, near_out, image_out):
    for c in range(near_out.shape[0]):
        near_out[c] = near_ref[:, c]
    image_out[...] = image_ref[...]


def body(groups, members, specs, emission, opacity, bin_extinction, entry, exit_cell, response):
    cells, bins, rays = emission.shape
    colours = response.shape[0]
    tiles = rays // (members * LANES)
    rows = padded(colours)
    f32 = jnp.float32
    vmem = pl.BlockSpec(memory_space=pltpu.VMEM)
    hbm = pl.BlockSpec(memory_space=pltpu.HBM)
    dma = pltpu.SemaphoreType.DMA
    near, image = pl.pallas_call(
        functools.partial(kernel, groups, members, specs),
        out_shape=(
            pltpu.VMEM((1, colours, rays), f32),
            pltpu.VMEM((colours, rays), f32),
        ),
        in_specs=[hbm] * 6,
        out_specs=(vmem, vmem),
        scratch_shapes=[
            pltpu.VMEM((2, tiles * members, cells, bins, LANES), emission.dtype),
            pltpu.VMEM((bins // SUBLANES, SUBLANES, LANES), f32),
            pltpu.VMEM((bins,), f32),
            pltpu.VMEM((2 * rays,), jnp.int32),
            pltpu.VMEM((colours, bins), f32),
            pltpu.VMEM((colours, bins, LANES), f32),
            pltpu.VMEM((specs, colours, bins, LANES), f32),
            pltpu.VMEM((tiles * members + 1, bins, LANES), f32),
            pltpu.VMEM((tiles, members * specs, bins, LANES), f32),
            pltpu.VMEM((tiles * members, bins, LANES), f32),
            pltpu.VMEM((tiles, members * specs, bins, LANES), f32),
            pltpu.VMEM((tiles, specs, bins, LANES), f32),
            pltpu.VMEM((tiles, specs, bins, LANES), f32),
            pltpu.VMEM((members, 2, rows * tiles, LANES), f32),
            pltpu.VMEM((members, 2, rows * tiles, LANES), f32),
            pltpu.VMEM((rows * tiles, LANES), f32),
            pltpu.VMEM((max(groups - 1, 1), members, rows * tiles, LANES), f32),
            pltpu.VMEM((members * specs, 2, rows * tiles, LANES), f32),
            dma((len(read_runs(tiles * members)),)), dma((3,)), dma, dma,
            dma, dma((tiles,)), dma, dma((tiles,)), dma, dma((tiles,)),
            dma, dma, dma((max(groups - 1, 1),)), dma((max(groups - 1, 1),)),
            pltpu.SemaphoreType.REGULAR,
        ],
        compiler_params=pltpu.CompilerParams(
            collective_id=0, has_side_effects=True, vmem_limit_bytes=56 * 2**20,
        ),
    )(emission, opacity, bin_extinction, entry, exit_cell, response)
    near, image = pl.pallas_call(
        place,
        out_shape=(
            jax.ShapeDtypeStruct((colours, 1, rays), f32),
            jax.ShapeDtypeStruct((colours, rays), f32),
        ),
        in_specs=[vmem, vmem],
        out_specs=(vmem, vmem),
    )(*(pltpu.with_memory_space_constraint(x, pltpu.VMEM) for x in (near, image)))
    return jnp.transpose(near, (1, 0, 2)), image


def solution(mesh):
    sections = mesh.shape["depth"]
    specs = mesh.shape["spec"]

    def program(emission, *rest):
        rays = emission.shape[2]
        members = max(
            m for m in range(1, sections + 1)
            if sections % m == 0 and rays % (m * LANES) == 0 and (2 * m <= sections or m == 1)
        )
        placed = (
            P("depth", "spec", None),
            P("depth", "spec", None),
            P("spec"),
            P(),
            P(),
            P(None, "spec"),
        )
        return jax.shard_map(
            functools.partial(body, sections // members, members, specs),
            mesh=mesh, in_specs=placed, out_specs=(P("depth", None, None), P()), check_vma=False,
        )(emission, *rest)

    return program
```

```python
import functools
import math
import jax
import jax.numpy as jnp
from jax import lax
from jax.experimental import pallas as pl
from jax.experimental.pallas import tpu as pltpu
from jax.sharding import PartitionSpec as P

LANES = 128
SUBLANES = 8
MESH = pl.DeviceIdType.MESH


def padded(colours):
    return -(-colours // 4) * 4


def read_runs(count):
    runs = []
    start = 0
    for length in (1, 1, 2, 4, *[8] * count):
        if start < count:
            runs.append((start, min(length, count - start)))
            start += length
    return runs


def column(row, eye):
    return jnp.sum(jnp.where(eye, row, 0.0), axis=1, keepdims=True)


def kernel(
    groups, members, specs,
    em_hbm, op_hbm, ext_hbm, entry_hbm, exit_hbm, resp_hbm,
    near_ref, image_ref,
    data_v, scale_v, ext_v, bounds_v, resp_v, w_own, w_all,
    s_out, s_in, l_out, l_in, d_out, d_in, f_out, f_in, x_out, x_in, shape_v,
    data_sem, small_sem, w_send, w_recv,
    s_send, s_recv, l_send, l_recv, d_send, d_recv, f_send, f_recv, x_send, x_recv, ready,
):
    cells, bins, rays = em_hbm.shape
    colours = resp_hbm.shape[0]
    tiles = rays // (members * LANES)
    rows = padded(colours)
    sections = groups * members
    cell_step = 1.0 / (cells * sections)
    me = lax.axis_index("depth")
    spec = lax.axis_index("spec")
    g = me // members
    mi = me % members
    lead = specs - 1
    is_lead = spec == lead
    last = members - 1
    paired = members & (members - 1) == 0

    def owner(t):
        return mi ^ (last - t) if paired else (mi + 1 + t) % members

    def when(condition, body):
        if condition is True:
            body()
        elif condition is not False:
            pl.when(condition)(body)

    def core(group, member, s):
        return (group * members + member, s)

    def lanes(j, q):
        return pl.ds(pl.multiple_of((j * members + q) * LANES, LANES), LANES)

    count = tiles * members
    ahead_first = (g < groups - 1) if groups > 1 and count % 2 == 0 else False

    def place_of(p):
        return p // members, p % members

    def read(n, hbm, p, sem):
        j, t = place_of(p)
        at = lanes(j, owner(t))
        return pltpu.make_async_copy(
            hbm.at[:, :, at], data_v.at[n, j * members + t], data_sem.at[sem]
        )

    runs = read_runs(count)

    def sem_of(pair):
        return next(n for n, (start, length) in enumerate(runs) if start <= pair < start + length)

    def read_wait(number, extra=True):
        for n, (start, length) in enumerate(runs):
            def wait():
                pairs = data_v.at[:, pl.ds(0, length)]
                pltpu.make_async_copy(pairs, pairs, data_sem.at[n]).wait()

            when((number == start) if extra is True else extra & (number == start), wait)

    together = jnp.logical_not(ahead_first) if ahead_first is not False else True

    first_read = read(0, op_hbm, 0, 0)
    first_read.start()

    small = [
        pltpu.make_async_copy(hbm, vmem, small_sem.at[n])
        for n, (hbm, vmem) in enumerate(
            ((ext_hbm, ext_v), (resp_hbm, resp_v))
        )
    ]
    for n, hbm in enumerate((entry_hbm, exit_hbm)):
        pltpu.make_async_copy(hbm, bounds_v.at[pl.ds(n * rays, rays)], small_sem.at[2]).start()
    for copy in small:
        copy.start()

    barrier = pltpu.get_barrier_semaphore()
    near_barrier = groups == 2

    def greet(group, member, s):
        pl.semaphore_signal(barrier, inc=1, device_id=core(group, member, s), device_id_type=MESH)

    if near_barrier:
        @pl.when(is_lead)
        def _():
            for s in range(specs - 1):
                greet(g, mi, s)

    def read_in_turn():
        for p in range(1, count):
            read(0, op_hbm, p, sem_of(p // 2)).start()
        for p in range(count):
            read(1, em_hbm, p, sem_of((count + p) // 2)).start()

    def read_together():
        for p in range(count):
            if p > 0:
                read(0, op_hbm, p, sem_of(p)).start()
            read(1, em_hbm, p, sem_of(p)).start()

    when(ahead_first, read_in_turn)
    when(together, read_together)

    if near_barrier:
        @pl.when(is_lead)
        def _():
            for t in range(last):
                for s in range(specs):
                    greet(g, owner(t), s)


            @pl.when(g == 0)
            def _():
                greet(1, mi, lead)
    else:
        @pl.loop(1, sections * specs)
        def _(n):
            index = (me * specs + spec + n) % (sections * specs)
            greet(index // (members * specs), index // specs % members, index % specs)

    def answer():
        pl.semaphore_signal(ready, inc=1, device_id=core(0, mi, lead), device_id_type=MESH)

    def enter():
        if near_barrier:
            @pl.when(is_lead & (g == 0))
            def _():
                if last > 0:
                    pl.semaphore_wait(barrier, last)

            @pl.when(is_lead & (g == 1))
            def _():
                pl.semaphore_wait(barrier, members)
                answer()

            @pl.when(spec != lead)
            def _():
                pl.semaphore_wait(barrier, members)
        else:
            pl.semaphore_wait(barrier, sections * specs - 1)

    pltpu.make_async_copy(bounds_v, bounds_v, small_sem.at[2]).wait()
    small[0].wait()

    eye = lax.broadcasted_iota(jnp.int32, (bins, bins), 0) == lax.broadcasted_iota(
        jnp.int32, (bins, bins), 1
    )
    scale = column(ext_v[...].reshape(1, bins), eye) * (-cell_step * math.log2(math.e))
    scale = jnp.broadcast_to(scale, (bins, LANES))
    scale_v[...] = scale.reshape(-1, SUBLANES, LANES)
    first = me * cells

    def bounds(j, t):
        at = (j * members + owner(t)) * LANES
        low = bounds_v[pl.ds(pl.multiple_of(at, LANES), LANES)].reshape(1, LANES) - first
        high = bounds_v[pl.ds(pl.multiple_of(rays + at, LANES), LANES)].reshape(1, LANES) - first
        low = jnp.broadcast_to(low, (SUBLANES, LANES))
        high = jnp.broadcast_to(high, (SUBLANES, LANES))
        return low, high

    def march(j, t, slot, entering, leaving):
        low, high = bounds(j, t)
        run = jnp.zeros(scale_v.shape, jnp.float32)
        glow = jnp.zeros(scale_v.shape, jnp.float32)
        for i in range(cells):
            dense = data_v[0, j * members + t, i].astype(jnp.float32).reshape(scale_v.shape)
            shine = data_v[1, j * members + t, i].astype(jnp.float32).reshape(scale_v.shape)
            if entering:
                entered = jnp.where(low <= i, 1.0, 0.0)
                dense = dense * entered[None]
            if entering and leaving:
                shine = shine * jnp.where(high > i, entered, 0.0)[None]
            elif entering:
                shine = shine * entered[None]
            elif leaving:
                shine = shine * jnp.where(high > i, 1.0, 0.0)[None]
            glow = glow + shine * jnp.exp2(run)
            run = run + dense * scale_v[...]
        s_out[slot] = run.reshape(bins, LANES)
        l_out[j * members + t] = (glow * cell_step).reshape(bins, LANES)

    def march_here(j, t, slot):
        if sections % 4:
            march(j, t, slot, True, True)
            return

        @pl.when(4 * me < sections)
        def _():
            march(j, t, slot, True, False)

        @pl.when((4 * me >= sections) & (4 * me < 3 * sections))
        def _():
            march(j, t, slot, False, False)

        @pl.when(4 * me >= 3 * sections)
        def _():
            march(j, t, slot, False, True)

    def depth_of(j, t, entering):
        low, _ = bounds(j, t)
        total = jnp.zeros(scale_v.shape, jnp.float32)
        for i in range(cells):
            dense = data_v[0, j * members + t, i].astype(jnp.float32).reshape(scale_v.shape)
            if entering:
                dense = dense * jnp.where(low <= i, 1.0, 0.0)[None]
            total = total + dense
        s_out[j * members + t] = (total * scale_v[...]).reshape(bins, LANES)

    def depth_here(j, t):
        if sections % 4:
            depth_of(j, t, True)
            return

        @pl.when(4 * me < sections)
        def _():
            depth_of(j, t, True)

        @pl.when(4 * me >= sections)
        def _():
            depth_of(j, t, False)

    def piece(out, into, send, recv, j, t):
        return pltpu.make_async_remote_copy(
            out.at[j * members + t], into.at[j, mi * specs + spec], send, recv.at[j],
            device_id=core(g, owner(t), lead), device_id_type=MESH,
        )

    def needed(j):
        return (g < groups - 1) | (mi < last) | (j == 0)

    def leaves(t):
        return (t < last) | (spec != lead)

    depth_args = (s_out, s_in, s_send, s_recv)
    light_args = (l_out, l_in, l_send, l_recv)

    def send(args, j, t):
        @pl.when(leaves(t))
        def _():
            piece(*args, j, t).start()

        @pl.when((t == last) & is_lead)
        def _():
            args[1][j, mi * specs + spec] = args[0][j * members + t]

    weights_copy = pltpu.make_async_remote_copy(
        w_own, w_all.at[spec], w_send, w_recv, device_id=(me, lead), device_id_type=MESH,
    )

    def landed(ref, recv):
        pltpu.make_async_remote_copy(
            ref, ref, w_send, recv, device_id=(me, lead), device_id_type=MESH
        ).wait_recv()

    def drained(ref, send):
        pltpu.make_async_remote_copy(
            ref, ref, send, w_recv, device_id=(me, lead), device_id_type=MESH
        ).wait_send()

    def depth_sent():
        @pl.when(is_lead)
        def _():
            drained(s_out.at[pl.ds(0, tiles * last)], s_send)

        @pl.when(spec != lead)
        def _():
            drained(s_out.at[pl.ds(0, count)], s_send)

    def first_pass():
        hold = jnp.minimum(count - 1, 4 + 2 * (last - mi))

        @pl.loop(0, count)
        def _(p):
            j, t = place_of(p)

            read_wait(p // 2, p % 2 == 0)
            depth_here(j, t)

            @pl.when(p == hold)
            def _():
                enter()

                @pl.loop(0, hold)
                def _(u):
                    send(depth_args, *place_of(u))

            @pl.when(p >= hold)
            def _():
                send(depth_args, j, t)

    when(ahead_first, first_pass)

    def second_pass():
        hold = 0 if ahead_first is False else jnp.where(ahead_first, count * 3 // 8, 0)

        def leave(u):
            j, t = place_of(u)

            def depth():
                send(depth_args, j, t)

            when(needed(j) if together is True else together & needed(j), depth)
            send(light_args, j, t)

        @pl.loop(0, count)
        def _(p):
            if ahead_first is False:
                read_wait(p)
                slot = p
            else:
                read_wait(jnp.where(together, p, (count + p) // 2), together | (p % 2 == 0))
                slot = jnp.where(together, p, count)
            march_here(*place_of(p), slot)

            @pl.when(p == hold)
            def _():
                when(together, enter)
                when(ahead_first, depth_sent)

                @pl.loop(0, hold)
                def _(u):
                    leave(u)

            @pl.when(p >= hold)
            def _():
                leave(p)

    second_pass()

    small[1].wait()
    for c in range(colours):
        w_own[c] = jnp.broadcast_to(column(resp_v[pl.ds(c, 1), :], eye), (bins, LANES))
    x_out[...] = jnp.zeros_like(x_out)
    f_out[...] = jnp.zeros_like(f_out)

    @pl.when(is_lead)
    def _():
        w_all[lead] = w_own[...]

    @pl.when(spec != lead)
    def _():
        weights_copy.start()

    def arrive(args, j):
        landed(args[1].at[j, pl.ds(0, members * specs - 1)], args[3].at[j])

    def arrive_depth(j):
        if j == 0:
            arrive(depth_args, j)
            return

        @pl.when(g < groups - 1)
        def _():
            arrive(depth_args, j)

        @pl.when((g == groups - 1) & (mi < last))
        def _():
            if last > 0:
                landed(s_in.at[j, pl.ds(0, last * specs - 1)], s_recv.at[j])

        @pl.when((g == groups - 1) & (mi == last))
        def _():
            if last > 0:
                landed(s_in.at[j, pl.ds(0, last * specs)], s_recv.at[j])

    def section(ref, j, k):
        return ref[j, pl.ds(k * specs, specs)]

    def chain_start(j):
        for s in range(specs):
            for v in range(0, bins, SUBLANES):
                at = (j, s, pl.ds(v, SUBLANES))
                pltpu.make_async_remote_copy(
                    d_out.at[at], d_in.at[at], d_send, d_recv.at[j],
                    device_id=core((g + 1) % groups, mi, lead), device_id_type=MESH,
                ).start()

    def chain_wait(j):
        landed(d_in.at[j], d_recv.at[j])

    def total_copy(dg, k, s):
        return pltpu.make_async_remote_copy(
            x_out, x_in.at[dg - 1, mi], x_send.at[dg - 1], x_recv.at[dg - 1],
            device_id=core((g + dg) % groups, k, s), device_id_type=MESH,
        )

    def block_copy(k, s):
        return pltpu.make_async_remote_copy(
            f_out.at[k], f_in.at[mi], f_send, f_recv,
            device_id=core(g, k, s), device_id_type=MESH,
        )

    @pl.when(is_lead)
    def _():
        for j in range(tiles):
            arrive_depth(j)

            if near_barrier and j == 0:
                @pl.when(g == 1)
                def _():
                    answer()

            @pl.when(g == 0)
            def _():
                d_in[j] = jnp.zeros(d_in.shape[1:], jnp.float32)

            if groups > 1:
                @pl.when(g < groups - 1)
                def _():
                    here = section(s_in, j, 0)
                    for k in range(1, members):
                        here = here + section(s_in, j, k)
                    if groups > 2:
                        @pl.when(g > 0)
                        def _():
                            chain_wait(j)

                        here = here + d_in[j]
                    d_out[j] = here
                    if near_barrier and j == 0:
                        pl.semaphore_wait(ready, 1)
                    chain_start(j)

        if specs > 1:
            landed(w_all.at[pl.ds(0, specs - 1)], w_recv)

        nearer = []

        def settle():
            for k, row, value in nearer:
                f_out[k, 0, pl.ds(row, 1), :] = jnp.sum(value, axis=0, keepdims=True)
            nearer.clear()

        for j in range(tiles):
            arrive(light_args, j)
            if groups > 1:
                @pl.when((g > 0) if groups == 2 else (g == groups - 1))
                def _():
                    chain_wait(j)

            ahead = d_in[j]
            sums = [jnp.zeros((SUBLANES, LANES), jnp.float32) for _ in range(colours)]
            for k in range(members):
                seen = jnp.exp2(ahead) * section(l_in, j, k)
                for c in range(colours):
                    if k > 0:
                        nearer.append((k, rows * j + c, sums[c]))
                    part = (seen * w_all[:, c]).reshape(-1, SUBLANES, LANES)
                    sums[c] = sums[c] + jnp.sum(part, axis=0)
                if k < members - 1:
                    ahead = ahead + section(s_in, j, k)
            for c in range(colours):
                x_out[pl.ds(rows * j + c, 1), :] = jnp.sum(sums[c], axis=0, keepdims=True)
            if j < tiles - 1:
                settle()

        if near_barrier:
            @pl.when(g == 0)
            def _():
                pl.semaphore_wait(ready, 1)

        for k in range(members):
            for dg in range(1, groups):
                for s in range(specs):
                    total_copy(dg, k, s).start()
        settle()
        for k in range(members):
            f_out[k, 1] = x_out[...]
        for k in range(members):
            for s in range(specs):
                @pl.when((k != mi) | (s != lead))
                def _():
                    block_copy(k, s).start()
        f_in[mi] = f_out[mi]

    @pl.when(is_lead)
    def _():
        landed(f_in.at[pl.ds(0, last)], f_recv)

    @pl.when(spec != lead)
    def _():
        landed(f_in, f_recv)

    for dg in range(1, groups):
        landed(x_in.at[dg - 1], x_recv.at[dg - 1])

    for q in range(members):
        near = f_in[q, 0]
        image = f_in[q, 1]
        for dg in range(1, groups):
            src = (g + groups - dg) % groups
            value = x_in[dg - 1, q]
            near = near + value * jnp.where(src < g, 1.0, 0.0)
            image = image + value
        for j in range(tiles):
            at = pl.ds((j * members + q) * LANES, LANES)
            near_ref[0, :, at] = near[rows * j:rows * j + colours]
            image_ref[:, at] = image[rows * j:rows * j + colours]
    when((mi < last) if together is True else together & (mi < last), depth_sent)

    @pl.when((g == groups - 1) & (mi == last))
    def _():
        @pl.when(is_lead)
        def _():
            if last > 0:
                drained(s_out.at[pl.ds(0, last)], s_send)

        @pl.when(spec != lead)
        def _():
            drained(s_out.at[pl.ds(0, members)], s_send)

    @pl.when(is_lead)
    def _():
        drained(l_out.at[pl.ds(0, tiles * last)], l_send)
        if groups > 1:
            @pl.when(g < groups - 1)
            def _():
                drained(d_out, d_send)
        drained(shape_v.at[pl.ds(0, members * specs - 1)], f_send)
        for dg in range(1, groups):
            drained(shape_v.at[:, 0], x_send.at[dg - 1])

    @pl.when(spec != lead)
    def _():
        drained(l_out, l_send)
        weights_copy.wait_send()


def place(near_ref, image_ref, near_out, image_out):
    for c in range(near_out.shape[0]):
        near_out[c] = near_ref[:, c]
    image_out[...] = image_ref[...]


def body(groups, members, specs, emission, opacity, bin_extinction, entry, exit_cell, response):
    cells, bins, rays = emission.shape
    colours = response.shape[0]
    tiles = rays // (members * LANES)
    rows = padded(colours)
    f32 = jnp.float32
    vmem = pl.BlockSpec(memory_space=pltpu.VMEM)
    hbm = pl.BlockSpec(memory_space=pltpu.HBM)
    dma = pltpu.SemaphoreType.DMA
    near, image = pl.pallas_call(
        functools.partial(kernel, groups, members, specs),
        out_shape=(
            pltpu.VMEM((1, colours, rays), f32),
            pltpu.VMEM((colours, rays), f32),
        ),
        in_specs=[hbm] * 6,
        out_specs=(vmem, vmem),
        scratch_shapes=[
            pltpu.VMEM((2, tiles * members, cells, bins, LANES), emission.dtype),
            pltpu.VMEM((bins // SUBLANES, SUBLANES, LANES), f32),
            pltpu.VMEM((bins,), f32),
            pltpu.VMEM((2 * rays,), jnp.int32),
            pltpu.VMEM((colours, bins), f32),
            pltpu.VMEM((colours, bins, LANES), f32),
            pltpu.VMEM((specs, colours, bins, LANES), f32),
            pltpu.VMEM((tiles * members + 1, bins, LANES), f32),
            pltpu.VMEM((tiles, members * specs, bins, LANES), f32),
            pltpu.VMEM((tiles * members, bins, LANES), f32),
            pltpu.VMEM((tiles, members * specs, bins, LANES), f32),
            pltpu.VMEM((tiles, specs, bins, LANES), f32),
            pltpu.VMEM((tiles, specs, bins, LANES), f32),
            pltpu.VMEM((members, 2, rows * tiles, LANES), f32),
            pltpu.VMEM((members, 2, rows * tiles, LANES), f32),
            pltpu.VMEM((rows * tiles, LANES), f32),
            pltpu.VMEM((max(groups - 1, 1), members, rows * tiles, LANES), f32),
            pltpu.VMEM((members * specs, 2, rows * tiles, LANES), f32),
            dma((len(read_runs(tiles * members)),)), dma((3,)), dma, dma,
            dma, dma((tiles,)), dma, dma((tiles,)), dma, dma((tiles,)),
            dma, dma, dma((max(groups - 1, 1),)), dma((max(groups - 1, 1),)),
            pltpu.SemaphoreType.REGULAR,
        ],
        compiler_params=pltpu.CompilerParams(
            collective_id=0, has_side_effects=True, vmem_limit_bytes=56 * 2**20,
        ),
    )(emission, opacity, bin_extinction, entry, exit_cell, response)
    near, image = pl.pallas_call(
        place,
        out_shape=(
            jax.ShapeDtypeStruct((colours, 1, rays), f32),
            jax.ShapeDtypeStruct((colours, rays), f32),
        ),
        in_specs=[vmem, vmem],
        out_specs=(vmem, vmem),
    )(*(pltpu.with_memory_space_constraint(x, pltpu.VMEM) for x in (near, image)))
    return jnp.transpose(near, (1, 0, 2)), image


def solution(mesh):
    sections = mesh.shape["depth"]
    specs = mesh.shape["spec"]

    def program(emission, *rest):
        rays = emission.shape[2]
        members = max(
            m for m in range(1, sections + 1)
            if sections % m == 0 and rays % (m * LANES) == 0 and (2 * m <= sections or m == 1)
        )
        placed = (
            P("depth", "spec", None),
            P("depth", "spec", None),
            P("spec"),
            P(),
            P(),
            P(None, "spec"),
        )
        return jax.shard_map(
            functools.partial(body, sections // members, members, specs),
            mesh=mesh, in_specs=placed, out_specs=(P("depth", None, None), P()), check_vma=False,
        )(emission, *rest)

    return program
```

```python
import functools
import math
import jax
import jax.numpy as jnp
from jax import lax
from jax.experimental import pallas as pl
from jax.experimental.pallas import tpu as pltpu
from jax.sharding import PartitionSpec as P

LANES = 128
SUBLANES = 8
MESH = pl.DeviceIdType.MESH


def padded(colours):
    return -(-colours // 4) * 4


def read_runs(count):
    runs = []
    start = 0
    for length in (1, 1, 2, 4, *[8] * count):
        if start < count:
            runs.append((start, min(length, count - start)))
            start += length
    return runs


def column(row, eye):
    return jnp.sum(jnp.where(eye, row, 0.0), axis=1, keepdims=True)


def kernel(
    groups, members, specs,
    em_hbm, op_hbm, ext_hbm, entry_hbm, exit_hbm, resp_hbm,
    near_ref, image_ref,
    data_v, scale_v, ext_v, bounds_v, resp_v, w_own, w_all,
    s_out, s_in, l_out, l_in, d_out, d_in, f_out, f_in, x_out, x_in, shape_v,
    data_sem, small_sem, w_send, w_recv,
    s_send, s_recv, l_send, l_recv, d_send, d_recv, f_send, f_recv, x_send, x_recv, ready,
):
    cells, bins, rays = em_hbm.shape
    colours = resp_hbm.shape[0]
    tiles = rays // (members * LANES)
    rows = padded(colours)
    sections = groups * members
    cell_step = 1.0 / (cells * sections)
    me = lax.axis_index("depth")
    spec = lax.axis_index("spec")
    g = me // members
    mi = me % members
    lead = specs - 1
    is_lead = spec == lead
    last = members - 1
    paired = members & (members - 1) == 0

    def owner(t):
        return mi ^ (last - t) if paired else (mi + 1 + t) % members

    def when(condition, body):
        if condition is True:
            body()
        elif condition is not False:
            pl.when(condition)(body)

    def core(group, member, s):
        return (group * members + member, s)

    def lanes(j, q):
        return pl.ds(pl.multiple_of((j * members + q) * LANES, LANES), LANES)

    count = tiles * members
    ahead_first = (g < groups - 1) if groups > 1 and count % 2 == 0 else False

    def place_of(p):
        return p // members, p % members

    def read(n, hbm, p, sem):
        j, t = place_of(p)
        at = lanes(j, owner(t))
        return pltpu.make_async_copy(
            hbm.at[:, :, at], data_v.at[n, j * members + t], data_sem.at[sem]
        )

    runs = read_runs(count)

    def sem_of(pair):
        return next(n for n, (start, length) in enumerate(runs) if start <= pair < start + length)

    def read_wait(number, extra=True):
        for n, (start, length) in enumerate(runs):
            def wait():
                pairs = data_v.at[:, pl.ds(0, length)]
                pltpu.make_async_copy(pairs, pairs, data_sem.at[n]).wait()

            when((number == start) if extra is True else extra & (number == start), wait)

    together = jnp.logical_not(ahead_first) if ahead_first is not False else True

    first_read = read(0, op_hbm, 0, 0)
    first_read.start()

    small = [
        pltpu.make_async_copy(hbm, vmem, small_sem.at[n])
        for n, (hbm, vmem) in enumerate(
            ((ext_hbm, ext_v), (resp_hbm, resp_v))
        )
    ]
    for n, hbm in enumerate((entry_hbm, exit_hbm)):
        pltpu.make_async_copy(hbm, bounds_v.at[pl.ds(n * rays, rays)], small_sem.at[2]).start()
    for copy in small:
        copy.start()

    barrier = pltpu.get_barrier_semaphore()
    near_barrier = groups == 2

    def greet(group, member, s):
        pl.semaphore_signal(barrier, inc=1, device_id=core(group, member, s), device_id_type=MESH)

    if near_barrier:
        @pl.when(is_lead)
        def _():
            for s in range(specs - 1):
                greet(g, mi, s)

    def read_in_turn():
        for p in range(1, count):
            read(0, op_hbm, p, sem_of(p // 2)).start()
        for p in range(count):
            read(1, em_hbm, p, sem_of((count + p) // 2)).start()

    def read_together():
        for p in range(count):
            if p > 0:
                read(0, op_hbm, p, sem_of(p)).start()
            read(1, em_hbm, p, sem_of(p)).start()

    when(ahead_first, read_in_turn)
    when(together, read_together)

    if near_barrier:
        @pl.when(is_lead)
        def _():
            for t in range(last):
                for s in range(specs):
                    greet(g, owner(t), s)


            @pl.when(g == 0)
            def _():
                greet(1, mi, lead)
    else:
        @pl.loop(1, sections * specs)
        def _(n):
            index = (me * specs + spec + n) % (sections * specs)
            greet(index // (members * specs), index // specs % members, index % specs)

    def answer():
        pl.semaphore_signal(ready, inc=1, device_id=core(0, mi, lead), device_id_type=MESH)

    def enter():
        if near_barrier:
            @pl.when(is_lead & (g == 0))
            def _():
                if last > 0:
                    pl.semaphore_wait(barrier, last)

            @pl.when(is_lead & (g == 1))
            def _():
                pl.semaphore_wait(barrier, members)
                answer()

            @pl.when(spec != lead)
            def _():
                pl.semaphore_wait(barrier, members)
        else:
            pl.semaphore_wait(barrier, sections * specs - 1)

    pltpu.make_async_copy(bounds_v, bounds_v, small_sem.at[2]).wait()
    small[0].wait()

    eye = lax.broadcasted_iota(jnp.int32, (bins, bins), 0) == lax.broadcasted_iota(
        jnp.int32, (bins, bins), 1
    )
    scale = column(ext_v[...].reshape(1, bins), eye) * (-cell_step * math.log2(math.e))
    scale = jnp.broadcast_to(scale, (bins, LANES))
    scale_v[...] = scale.reshape(-1, SUBLANES, LANES)
    first = me * cells

    def bounds(j, t):
        at = (j * members + owner(t)) * LANES
        low = bounds_v[pl.ds(pl.multiple_of(at, LANES), LANES)].reshape(1, LANES) - first
        high = bounds_v[pl.ds(pl.multiple_of(rays + at, LANES), LANES)].reshape(1, LANES) - first
        low = jnp.broadcast_to(low, (SUBLANES, LANES))
        high = jnp.broadcast_to(high, (SUBLANES, LANES))
        return low, high

    def march(j, t, slot, entering, leaving):
        low, high = bounds(j, t)
        run = jnp.zeros(scale_v.shape, jnp.float32)
        glow = jnp.zeros(scale_v.shape, jnp.float32)
        for i in range(cells):
            dense = data_v[0, j * members + t, i].astype(jnp.float32).reshape(scale_v.shape)
            shine = data_v[1, j * members + t, i].astype(jnp.float32).reshape(scale_v.shape)
            if entering:
                entered = jnp.where(low <= i, 1.0, 0.0)
                dense = dense * entered[None]
            if entering and leaving:
                shine = shine * jnp.where(high > i, entered, 0.0)[None]
            elif entering:
                shine = shine * entered[None]
            elif leaving:
                shine = shine * jnp.where(high > i, 1.0, 0.0)[None]
            glow = glow + shine * jnp.exp2(run)
            run = run + dense * scale_v[...]
        s_out[slot] = run.reshape(bins, LANES)
        l_out[j * members + t] = (glow * cell_step).reshape(bins, LANES)

    def march_here(j, t, slot):
        if sections % 4:
            march(j, t, slot, True, True)
            return

        @pl.when(4 * me < sections)
        def _():
            march(j, t, slot, True, False)

        @pl.when((4 * me >= sections) & (4 * me < 3 * sections))
        def _():
            march(j, t, slot, False, False)

        @pl.when(4 * me >= 3 * sections)
        def _():
            march(j, t, slot, False, True)

    def depth_of(j, t, entering):
        low, _ = bounds(j, t)
        total = jnp.zeros(scale_v.shape, jnp.float32)
        for i in range(cells):
            dense = data_v[0, j * members + t, i].astype(jnp.float32).reshape(scale_v.shape)
            if entering:
                dense = dense * jnp.where(low <= i, 1.0, 0.0)[None]
            total = total + dense
        s_out[j * members + t] = (total * scale_v[...]).reshape(bins, LANES)

    def depth_here(j, t):
        if sections % 4:
            depth_of(j, t, True)
            return

        @pl.when(4 * me < sections)
        def _():
            depth_of(j, t, True)

        @pl.when(4 * me >= sections)
        def _():
            depth_of(j, t, False)

    def piece(out, into, send, recv, j, t):
        return pltpu.make_async_remote_copy(
            out.at[j * members + t], into.at[j, mi * specs + spec], send, recv.at[j],
            device_id=core(g, owner(t), lead), device_id_type=MESH,
        )

    def needed(j):
        return (g < groups - 1) | (mi < last) | (j == 0)

    def leaves(t):
        return (t < last) | (spec != lead)

    depth_args = (s_out, s_in, s_send, s_recv)
    light_args = (l_out, l_in, l_send, l_recv)

    def send(args, j, t):
        @pl.when(leaves(t))
        def _():
            piece(*args, j, t).start()

        @pl.when((t == last) & is_lead)
        def _():
            args[1][j, mi * specs + spec] = args[0][j * members + t]

    weights_copy = pltpu.make_async_remote_copy(
        w_own, w_all.at[spec], w_send, w_recv, device_id=(me, lead), device_id_type=MESH,
    )

    def landed(ref, recv):
        pltpu.make_async_remote_copy(
            ref, ref, w_send, recv, device_id=(me, lead), device_id_type=MESH
        ).wait_recv()

    def drained(ref, send):
        pltpu.make_async_remote_copy(
            ref, ref, send, w_recv, device_id=(me, lead), device_id_type=MESH
        ).wait_send()

    def depth_sent():
        @pl.when(is_lead)
        def _():
            drained(s_out.at[pl.ds(0, tiles * last)], s_send)

        @pl.when(spec != lead)
        def _():
            drained(s_out.at[pl.ds(0, count)], s_send)

    def first_pass():
        hold = jnp.minimum(count - 1, 4 + 2 * (last - mi))

        @pl.loop(0, count)
        def _(p):
            j, t = place_of(p)

            read_wait(p // 2, p % 2 == 0)
            depth_here(j, t)

            @pl.when(p == hold)
            def _():
                enter()

                @pl.loop(0, hold)
                def _(u):
                    send(depth_args, *place_of(u))

            @pl.when(p >= hold)
            def _():
                send(depth_args, j, t)

    when(ahead_first, first_pass)

    def second_pass():
        hold = 0 if ahead_first is False else jnp.where(ahead_first, count * 3 // 8, 0)

        def leave(u):
            j, t = place_of(u)

            def depth():
                send(depth_args, j, t)

            when(needed(j) if together is True else together & needed(j), depth)
            send(light_args, j, t)

        late = count // 2
        prompt = jnp.where(is_lead & together, jnp.maximum(hold, count * 3 // 8), count)

        @pl.loop(0, count)
        def _(p):
            if ahead_first is False:
                read_wait(p)
                slot = p
            else:
                read_wait(jnp.where(together, p, (count + p) // 2), together | (p % 2 == 0))
                slot = jnp.where(together, p, count)
            march_here(*place_of(p), slot)

            @pl.when(p == hold)
            def _():
                when(together, enter)
                when(ahead_first, depth_sent)

                @pl.loop(0, hold)
                def _(u):
                    leave(u)

            @pl.when((p >= hold) & (p < prompt))
            def _():
                leave(p)

            @pl.when(p - late >= prompt)
            def _():
                leave(p - late)

        @pl.loop(jnp.minimum(count, jnp.maximum(prompt, count - late)), count)
        def _(u):
            leave(u)

    second_pass()

    small[1].wait()
    for c in range(colours):
        w_own[c] = jnp.broadcast_to(column(resp_v[pl.ds(c, 1), :], eye), (bins, LANES))
    x_out[...] = jnp.zeros_like(x_out)
    f_out[...] = jnp.zeros_like(f_out)

    @pl.when(is_lead)
    def _():
        w_all[lead] = w_own[...]

    @pl.when(spec != lead)
    def _():
        weights_copy.start()

    def arrive(args, j):
        landed(args[1].at[j, pl.ds(0, members * specs - 1)], args[3].at[j])

    def arrive_depth(j):
        if j == 0:
            arrive(depth_args, j)
            return

        @pl.when(g < groups - 1)
        def _():
            arrive(depth_args, j)

        @pl.when((g == groups - 1) & (mi < last))
        def _():
            if last > 0:
                landed(s_in.at[j, pl.ds(0, last * specs - 1)], s_recv.at[j])

        @pl.when((g == groups - 1) & (mi == last))
        def _():
            if last > 0:
                landed(s_in.at[j, pl.ds(0, last * specs)], s_recv.at[j])

    def section(ref, j, k):
        return ref[j, pl.ds(k * specs, specs)]

    def chain_start(j):
        for s in range(specs):
            for v in range(0, bins, SUBLANES):
                at = (j, s, pl.ds(v, SUBLANES))
                pltpu.make_async_remote_copy(
                    d_out.at[at], d_in.at[at], d_send, d_recv.at[j],
                    device_id=core((g + 1) % groups, mi, lead), device_id_type=MESH,
                ).start()

    def chain_wait(j):
        landed(d_in.at[j], d_recv.at[j])

    def total_copy(dg, k, s):
        return pltpu.make_async_remote_copy(
            x_out, x_in.at[dg - 1, mi], x_send.at[dg - 1], x_recv.at[dg - 1],
            device_id=core((g + dg) % groups, k, s), device_id_type=MESH,
        )

    def block_copy(k, s):
        return pltpu.make_async_remote_copy(
            f_out.at[k], f_in.at[mi], f_send, f_recv,
            device_id=core(g, k, s), device_id_type=MESH,
        )

    @pl.when(is_lead)
    def _():
        for j in range(tiles):
            arrive_depth(j)

            if near_barrier and j == 0:
                @pl.when(g == 1)
                def _():
                    answer()

            @pl.when(g == 0)
            def _():
                d_in[j] = jnp.zeros(d_in.shape[1:], jnp.float32)

            if groups > 1:
                @pl.when(g < groups - 1)
                def _():
                    here = section(s_in, j, 0)
                    for k in range(1, members):
                        here = here + section(s_in, j, k)
                    if groups > 2:
                        @pl.when(g > 0)
                        def _():
                            chain_wait(j)

                        here = here + d_in[j]
                    d_out[j] = here
                    if near_barrier and j == 0:
                        pl.semaphore_wait(ready, 1)
                    chain_start(j)

        if specs > 1:
            landed(w_all.at[pl.ds(0, specs - 1)], w_recv)

        nearer = []

        def settle():
            for k, row, value in nearer:
                f_out[k, 0, pl.ds(row, 1), :] = jnp.sum(value, axis=0, keepdims=True)
            nearer.clear()

        for j in range(tiles):
            arrive(light_args, j)
            if groups > 1:
                @pl.when((g > 0) if groups == 2 else (g == groups - 1))
                def _():
                    chain_wait(j)

            ahead = d_in[j]
            sums = [jnp.zeros((SUBLANES, LANES), jnp.float32) for _ in range(colours)]
            for k in range(members):
                seen = jnp.exp2(ahead) * section(l_in, j, k)
                for c in range(colours):
                    if k > 0:
                        nearer.append((k, rows * j + c, sums[c]))
                    part = (seen * w_all[:, c]).reshape(-1, SUBLANES, LANES)
                    sums[c] = sums[c] + jnp.sum(part, axis=0)
                if k < members - 1:
                    ahead = ahead + section(s_in, j, k)
            for c in range(colours):
                x_out[pl.ds(rows * j + c, 1), :] = jnp.sum(sums[c], axis=0, keepdims=True)
            if j < tiles - 1:
                settle()

        if near_barrier:
            @pl.when(g == 0)
            def _():
                pl.semaphore_wait(ready, 1)

        for k in range(members):
            for dg in range(1, groups):
                for s in range(specs):
                    total_copy(dg, k, s).start()
        settle()
        for k in range(members):
            f_out[k, 1] = x_out[...]
        for k in range(members):
            for s in range(specs):
                @pl.when((k != mi) | (s != lead))
                def _():
                    block_copy(k, s).start()
        f_in[mi] = f_out[mi]

    @pl.when(is_lead)
    def _():
        landed(f_in.at[pl.ds(0, last)], f_recv)

    @pl.when(spec != lead)
    def _():
        landed(f_in, f_recv)

    for dg in range(1, groups):
        landed(x_in.at[dg - 1], x_recv.at[dg - 1])

    for q in range(members):
        near = f_in[q, 0]
        image = f_in[q, 1]
        for dg in range(1, groups):
            src = (g + groups - dg) % groups
            value = x_in[dg - 1, q]
            near = near + value * jnp.where(src < g, 1.0, 0.0)
            image = image + value
        for j in range(tiles):
            at = pl.ds((j * members + q) * LANES, LANES)
            near_ref[0, :, at] = near[rows * j:rows * j + colours]
            image_ref[:, at] = image[rows * j:rows * j + colours]
    when((mi < last) if together is True else together & (mi < last), depth_sent)

    @pl.when((g == groups - 1) & (mi == last))
    def _():
        @pl.when(is_lead)
        def _():
            if last > 0:
                drained(s_out.at[pl.ds(0, last)], s_send)

        @pl.when(spec != lead)
        def _():
            drained(s_out.at[pl.ds(0, members)], s_send)

    @pl.when(is_lead)
    def _():
        drained(l_out.at[pl.ds(0, tiles * last)], l_send)
        if groups > 1:
            @pl.when(g < groups - 1)
            def _():
                drained(d_out, d_send)
        drained(shape_v.at[pl.ds(0, members * specs - 1)], f_send)
        for dg in range(1, groups):
            drained(shape_v.at[:, 0], x_send.at[dg - 1])

    @pl.when(spec != lead)
    def _():
        drained(l_out, l_send)
        weights_copy.wait_send()


def place(near_ref, image_ref, near_out, image_out):
    for c in range(near_out.shape[0]):
        near_out[c] = near_ref[:, c]
    image_out[...] = image_ref[...]


def body(groups, members, specs, emission, opacity, bin_extinction, entry, exit_cell, response):
    cells, bins, rays = emission.shape
    colours = response.shape[0]
    tiles = rays // (members * LANES)
    rows = padded(colours)
    f32 = jnp.float32
    vmem = pl.BlockSpec(memory_space=pltpu.VMEM)
    hbm = pl.BlockSpec(memory_space=pltpu.HBM)
    dma = pltpu.SemaphoreType.DMA
    near, image = pl.pallas_call(
        functools.partial(kernel, groups, members, specs),
        out_shape=(
            pltpu.VMEM((1, colours, rays), f32),
            pltpu.VMEM((colours, rays), f32),
        ),
        in_specs=[hbm] * 6,
        out_specs=(vmem, vmem),
        scratch_shapes=[
            pltpu.VMEM((2, tiles * members, cells, bins, LANES), emission.dtype),
            pltpu.VMEM((bins // SUBLANES, SUBLANES, LANES), f32),
            pltpu.VMEM((bins,), f32),
            pltpu.VMEM((2 * rays,), jnp.int32),
            pltpu.VMEM((colours, bins), f32),
            pltpu.VMEM((colours, bins, LANES), f32),
            pltpu.VMEM((specs, colours, bins, LANES), f32),
            pltpu.VMEM((tiles * members + 1, bins, LANES), f32),
            pltpu.VMEM((tiles, members * specs, bins, LANES), f32),
            pltpu.VMEM((tiles * members, bins, LANES), f32),
            pltpu.VMEM((tiles, members * specs, bins, LANES), f32),
            pltpu.VMEM((tiles, specs, bins, LANES), f32),
            pltpu.VMEM((tiles, specs, bins, LANES), f32),
            pltpu.VMEM((members, 2, rows * tiles, LANES), f32),
            pltpu.VMEM((members, 2, rows * tiles, LANES), f32),
            pltpu.VMEM((rows * tiles, LANES), f32),
            pltpu.VMEM((max(groups - 1, 1), members, rows * tiles, LANES), f32),
            pltpu.VMEM((members * specs, 2, rows * tiles, LANES), f32),
            dma((len(read_runs(tiles * members)),)), dma((3,)), dma, dma,
            dma, dma((tiles,)), dma, dma((tiles,)), dma, dma((tiles,)),
            dma, dma, dma((max(groups - 1, 1),)), dma((max(groups - 1, 1),)),
            pltpu.SemaphoreType.REGULAR,
        ],
        compiler_params=pltpu.CompilerParams(
            collective_id=0, has_side_effects=True, vmem_limit_bytes=56 * 2**20,
        ),
    )(emission, opacity, bin_extinction, entry, exit_cell, response)
    near, image = pl.pallas_call(
        place,
        out_shape=(
            jax.ShapeDtypeStruct((colours, 1, rays), f32),
            jax.ShapeDtypeStruct((colours, rays), f32),
        ),
        in_specs=[vmem, vmem],
        out_specs=(vmem, vmem),
    )(*(pltpu.with_memory_space_constraint(x, pltpu.VMEM) for x in (near, image)))
    return jnp.transpose(near, (1, 0, 2)), image


def solution(mesh):
    sections = mesh.shape["depth"]
    specs = mesh.shape["spec"]

    def program(emission, *rest):
        rays = emission.shape[2]
        members = max(
            m for m in range(1, sections + 1)
            if sections % m == 0 and rays % (m * LANES) == 0 and (2 * m <= sections or m == 1)
        )
        placed = (
            P("depth", "spec", None),
            P("depth", "spec", None),
            P("spec"),
            P(),
            P(),
            P(None, "spec"),
        )
        return jax.shard_map(
            functools.partial(body, sections // members, members, specs),
            mesh=mesh, in_specs=placed, out_specs=(P("depth", None, None), P()), check_vma=False,
        )(emission, *rest)

    return program
```
